128 devices in a mesh: row: 16 (over z, y), col: 8 (over x, core).
Axes of the slice: x: 4, y: 4, z: 4, core: 2. Of those that a mesh axis runs over, the one named last changes fastest.
Arguments:
- inv_interior: bfloat16 [512, 1024, 1024], P(('row', 'col')), may hold values from -1 to 3
- coupling: bfloat16 [512, 1024, 512], P(('row', 'col')), may hold values from -0.375 to 0.375
- boundary_stiff: bfloat16 [512, 512, 512], P(('row', 'col')), may hold values from -6 to 6
- mass_interior: float32 [512, 1024], P(('row', 'col')), may hold values from 0.5 to 2
- mass_boundary: float32 [512, 512], P(('row', 'col')), may hold values from 0.5 to 2
- block_map: int32 [512, 4], P(('row', 'col')), may hold values from 0 to 127, as said below
- modes: bfloat16 [16384, 1024], P('col', 'row'), may hold values from -0.046875 to 0.046875
Outputs:
- iface_stiff: bfloat16 [16384, 16384], P('row', 'col')
- iface_mass: bfloat16 [16384, 16384], P('row', 'col')
- reduced_stiff: float32 [1024, 1024], P(('row', 'col'))
- reduced_mass: float32 [1024, 1024], P(('row', 'col'))
- mass_diagonal: float32 [16384], P(('row', 'col'))
The draws below stay inside these ranges and needn't reach their ends.
Inputs may be any that keep to these rules, and one draw needn't show every extreme that they name: Interface block p belongs to tile row p // 8 and tile column p // 16; the pair (block_map[s, a], block_map[s, b]) belongs to the tile of its row's tile row and its column's tile column. Over the 4 substructures of one device (aligned blocks of rows), no two triples (s, a, b) fall into the same tile, and in every draw some tile receives a pair from every device.
All inputs are finite; a program needn't handle non-finite values.
Results may differ from the reference program's by a relative error of at most 0.0058.
Values may be sent and summed in bfloat16 or wider, within the bound.
A program may use at most 192 MiB of HBM per device.

```python
import math
import jax
import jax.numpy as jnp
from jax import lax

NI = 1024
NBD = 512
BLK = 128
NIF = 16384
NM = 1024
NB = 4
NBLK = 128
SUBS = 512
TILE_ROWS = 1024
TILE_COLS = 2048


def draw_inv_interior(key, part):
    diag_key, noise_key = jax.random.split(jax.random.fold_in(key, 11))
    diagonal = jax.random.uniform(diag_key, (SUBS, NI), jnp.float32, 0.5, 2.0)
    noise = jax.random.normal(noise_key, (SUBS, NI, NI), jnp.float32) * (0.5 / math.sqrt(NI))
    symmetric = (noise + jnp.swapaxes(noise, 1, 2)) * (1.0 / math.sqrt(2.0))
    whole = symmetric + diagonal[:, :, None] * jnp.eye(NI, dtype=jnp.float32)[None, :, :]
    return whole.astype(jnp.bfloat16)


def fix_first(order, common_col):
    position = jnp.argmax(order == common_col).astype(jnp.int32)
    return order.at[position].set(order[0]).at[0].set(common_col)


def draw_block_map(key, part):
    row_groups = NIF // TILE_ROWS
    col_groups = NIF // TILE_COLS
    device_count = row_groups * col_groups
    per_col = row_groups // col_groups
    group_blocks = TILE_ROWS // BLK
    base = jax.random.fold_in(key, 23)
    common_key, order_key, offset_key = jax.random.split(base, 3)
    common_col = jax.random.randint(common_key, (), 0, col_groups).astype(jnp.int32)
    order_keys = jax.random.split(order_key, device_count * per_col)
    orders = jax.vmap(lambda single: jax.random.permutation(single, col_groups))(order_keys).astype(jnp.int32)
    orders = orders.reshape(device_count, per_col, col_groups)
    leading = jax.vmap(fix_first, in_axes=(0, None))(orders[:, 0, :], common_col)
    orders = orders.at[:, 0, :].set(leading)
    parity = jnp.arange(per_col, dtype=jnp.int32)[None, :, None]
    groups = (orders * per_col + parity).reshape(device_count, per_col * col_groups)
    offsets = jax.random.randint(offset_key, (device_count, per_col * col_groups), 0, group_blocks).astype(jnp.int32)
    blocks = groups * group_blocks + offsets
    return blocks.reshape(SUBS, NB).astype(jnp.int32)


def steps_of(rng, dims, cuts, least, high):
    def one(dim, shards_of):
        heights = jax.random.uniform(jax.random.fold_in(jax.random.fold_in(rng, 6), dim), (shards_of,), jnp.float32, least / len(cuts), high / len(cuts))
        return jnp.repeat(jnp.exp(heights), dims[dim] // shards_of).reshape((-1,) + (1,) * (len(dims) - dim - 1))

    level = one(*cuts[0])
    for cut in cuts[1:]:
        level = level * one(*cut)
    return level


def normal_values(rng, dims, spread, bound, shards=(), kind=jnp.bfloat16):
    values = spread * jax.random.normal(rng, dims, jnp.float32)
    if shards:
        values = values * steps_of(rng, dims, shards, -0.22, 0.18)
    return jnp.clip(values, -bound, bound).astype(kind)


def setup_inputs(seed: int = 0) -> dict:
    key_of = jax.random.split(jax.random.key(seed), 8)
    return {
        "inv_interior": draw_inv_interior(jax.random.fold_in(key_of[7], 71), 0),
        "coupling": normal_values(key_of[1], (SUBS, NI, NBD), (NI // 4) ** -0.5, 0.375, ((0, 128),)),
        "boundary_stiff": normal_values(key_of[2], (SUBS, NBD, NBD), 1.0, 6.0, ((0, 128),)),
        "mass_interior": jnp.clip(jnp.exp(math.log(2.0) - 1.3862944 * jax.random.uniform(key_of[3], (SUBS, NI), jnp.float32) ** steps_of(key_of[3], (SUBS, NI), ((0, 128),), -0.2, 0.2)), 0.5, 2.0),
        "mass_boundary": jnp.clip(jnp.exp(math.log(2.0) - 1.3862944 * jax.random.uniform(key_of[4], (SUBS, NBD), jnp.float32) ** steps_of(key_of[4], (SUBS, NBD), ((0, 128),), -0.2, 0.2)), 0.5, 2.0),
        "block_map": draw_block_map(jax.random.fold_in(key_of[7], 71), 0),
        "modes": normal_values(key_of[6], (NIF, NM), NIF ** -0.5, 0.046875, ((0, 8), (1, 16))),
    }


def condense(pieces):
    inverse, couple, stiffness, interior_mass, boundary_mass = pieces
    static_modes = (-jnp.dot(inverse, couple, preferred_element_type=jnp.float32)).astype(jnp.bfloat16)
    stiff_cond = stiffness.astype(jnp.float32) + jnp.dot(couple.T, static_modes, preferred_element_type=jnp.float32)
    weighted = (static_modes.astype(jnp.float32) * interior_mass[:, None]).astype(jnp.bfloat16)
    mass_cond = jnp.dot(static_modes.T, weighted, preferred_element_type=jnp.float32) + jnp.diag(boundary_mass)
    return jnp.stack([stiff_cond, mass_cond])


def reference(inv_interior, coupling, boundary_stiff, mass_interior, mass_boundary, block_map, modes):
    condensed = lax.map(condense, (inv_interior, coupling, boundary_stiff, mass_interior, mass_boundary))
    blocks = condensed.reshape(SUBS, 2, NB, BLK, NB, BLK).transpose(0, 2, 4, 1, 3, 5)
    block_rows = jnp.broadcast_to(block_map[:, :, None], (SUBS, NB, NB))
    block_cols = jnp.broadcast_to(block_map[:, None, :], (SUBS, NB, NB))
    assembled = jnp.zeros((NBLK, NBLK, 2, BLK, BLK), jnp.float32).at[block_rows, block_cols].add(blocks)
    full_pair = assembled.transpose(2, 0, 3, 1, 4).reshape(2, NIF, NIF)
    iface_stiff = full_pair[0].astype(jnp.bfloat16)
    mass_full = full_pair[1]
    mass_diagonal = jnp.diagonal(mass_full)
    positions = jnp.arange(NIF, dtype=jnp.int32)
    iface_mass = mass_full.at[positions, positions].set(jnp.float32(0.0)).astype(jnp.bfloat16)
    modes_exact = modes.astype(jnp.float32)
    stiff_image = jnp.dot(iface_stiff, modes, preferred_element_type=jnp.float32)
    mass_image = jnp.dot(iface_mass, modes, preferred_element_type=jnp.float32) + mass_diagonal[:, None] * modes_exact
    image = jnp.concatenate([stiff_image, mass_image], 1)
    reduced = jnp.dot(modes_exact.T, image, precision=lax.Precision.HIGHEST, preferred_element_type=jnp.float32)
    return iface_stiff, iface_mass, reduced[:, :NM], reduced[:, NM:], mass_diagonal
```

```python
import functools

import jax
import jax.numpy as jnp
from jax import lax
from jax.experimental import pallas as pl
from jax.experimental.pallas import tpu as pltpu
from jax.sharding import PartitionSpec as P

MESH = pl.DeviceIdType.MESH
BLK = 128
F32 = jnp.float32
BF16 = jnp.bfloat16
I32 = jnp.int32
ANY = pl.BlockSpec(memory_space=pl.ANY)
VMEM = pl.BlockSpec(memory_space=pltpu.VMEM)
DMA = pltpu.SemaphoreType.DMA
ROW_OFFS = [(dz, dy) for dz in range(4) for dy in range(4)]
COL_OFFS = [(dx, dk) for dx in range(4) for dk in range(2)]


class Place:
    def __init__(self):
        self.row = lax.axis_index("row")
        self.col = lax.axis_index("col")
        self.z, self.y = lax.div(self.row, 4), lax.rem(self.row, 4)
        self.x, self.k = lax.div(self.col, 2), lax.rem(self.col, 2)

    def row_at(self, dz, dy):
        return lax.rem(self.z + dz, 4) * 4 + lax.rem(self.y + dy, 4)

    def col_at(self, dx, dk):
        return lax.rem(self.x + dx, 4) * 2 + lax.rem(self.k + dk, 2)


def condense_kernel(
    map_ref, inv_ref, couple_ref, stiff_ref, mi_ref, mb_ref, a_ref, b_ref, ma_ref, mb_out_ref
):
    s = pl.program_id(0)
    inverse = inv_ref[0]
    couple = couple_ref[0]
    static = (-jnp.dot(inverse, couple, preferred_element_type=F32)).astype(BF16)
    stiff = stiff_ref[0].astype(F32) + lax.dot_general(
        couple, static, (((0,), (0,)), ((), ())), preferred_element_type=F32
    )
    static_t = static.T
    weighted_t = (static_t.astype(F32) * mi_ref[0]).astype(BF16)
    mass = lax.dot_general(
        static_t, weighted_t, (((1,), (1,)), ((), ())), preferred_element_type=F32
    )
    width = mass.shape[0]
    row_ids = lax.broadcasted_iota(I32, (width, width), 0)
    col_ids = lax.broadcasted_iota(I32, (width, width), 1)
    mass = mass + jnp.where(row_ids == col_ids, mb_ref[0], F32(0.0))
    stiff = stiff.astype(BF16)
    mass = mass.astype(BF16)
    lines = lax.broadcasted_iota(I32, (8, BLK), 0)
    ids = [map_ref[s, a] for a in range(4)]
    table = jnp.zeros((8, BLK), I32)
    for a in range(4):
        table = jnp.where(lines == a, ids[a], table)
    for a in range(4):
        own = jnp.where(lines >= 4, ids[a], table)
        tile_row = ids[a] // 8
        a_ref[tile_row] = stiff[a * BLK : (a + 1) * BLK, :]
        ma_ref[tile_row] = own
        b_ref[tile_row] = mass[:, a * BLK : (a + 1) * BLK]
        mb_out_ref[tile_row] = own


def condense(inv_interior, coupling, boundary_stiff, mass_interior, mass_boundary, block_map):
    subs, inner, edge = coupling.shape
    return pl.pallas_call(
        condense_kernel,
        grid_spec=pltpu.PrefetchScalarGridSpec(
            num_scalar_prefetch=1,
            grid=(subs,),
            in_specs=[
                pl.BlockSpec((1, inner, inner), lambda s, m: (s, 0, 0)),
                pl.BlockSpec((1, inner, edge), lambda s, m: (s, 0, 0)),
                pl.BlockSpec((1, edge, edge), lambda s, m: (s, 0, 0)),
                pl.BlockSpec((1, 1, inner), lambda s, m: (s, 0, 0)),
                pl.BlockSpec((1, 1, edge), lambda s, m: (s, 0, 0)),
            ],
            out_specs=[
                pl.BlockSpec((16, BLK, edge), lambda s, m: (0, 0, 0)),
                pl.BlockSpec((16, edge, BLK), lambda s, m: (0, 0, 0)),
                pl.BlockSpec((16, 8, BLK), lambda s, m: (0, 0, 0)),
                pl.BlockSpec((16, 8, BLK), lambda s, m: (0, 0, 0)),
            ],
        ),
        out_shape=[
            jax.ShapeDtypeStruct((16, BLK, edge), BF16),
            jax.ShapeDtypeStruct((16, edge, BLK), BF16),
            jax.ShapeDtypeStruct((16, 8, BLK), I32),
            jax.ShapeDtypeStruct((16, 8, BLK), I32),
        ],
        name="condense",
    )(
        block_map,
        inv_interior,
        coupling,
        boundary_stiff,
        mass_interior.reshape(subs, 1, inner),
        mass_boundary.reshape(subs, 1, edge),
    )


def exchange_kernel(
    a1, b1, ma1, mb1, modes_t,
    a2, b2, ma2, mb2, cm, rm,
    arr_a, arr_b, arr_ma, arr_mb, pk_a, pk_b, pk_ma, pk_mb,
    a1s, a1r, b1s, b1r, ma1s, ma1r, mb1s, mb1r,
    a2s, a2r, b2s, b2r, ma2s, ma2r, mb2s, mb2r,
    m1s, m1r, m2s, m2r, chs, chr_, sbs, sbr, local,
):
    at = Place()
    row, col = at.row, at.col

    def remote(src, dst, ssem, rsem, r, c):
        return pltpu.make_async_remote_copy(
            src_ref=src, dst_ref=dst, send_sem=ssem, recv_sem=rsem,
            device_id=(r, c), device_id_type=MESH,
        )

    barrier = pltpu.get_barrier_semaphore()
    for dz, dy in ROW_OFFS[1:]:
        pl.semaphore_signal(barrier, inc=1, device_id=(at.row_at(dz, dy), col), device_id_type=MESH)
    for dx, dk in COL_OFFS[1:]:
        pl.semaphore_signal(barrier, inc=1, device_id=(row, at.col_at(dx, dk)), device_id_type=MESH)

    locals_ = [
        pltpu.make_async_copy(a1.at[row], arr_a.at[0], local.at[0]),
        pltpu.make_async_copy(b1.at[pl.ds(2 * col, 2)], arr_b.at[0], local.at[1]),
        pltpu.make_async_copy(ma1.at[row], arr_ma.at[0], local.at[2]),
        pltpu.make_async_copy(mb1.at[pl.ds(2 * col, 2)], arr_mb.at[0], local.at[3]),
        pltpu.make_async_copy(modes_t.at[:, pl.ds(0, 1024)], cm.at[0, row], local.at[4]),
        pltpu.make_async_copy(modes_t.at[:, pl.ds(1024, 1024)], cm.at[1, row], local.at[5]),
    ]
    for copy in locals_:
        copy.start()
    pl.semaphore_wait(barrier, 22)

    sends = []

    def go(copy):
        copy.start()
        sends.append(copy)
        return copy

    first = []
    for d in (1, 3, 2):
        for h in range(2):
            r = at.row_at(d, 0) if h == 0 else at.row_at(0, d)
            n = h * 3 + d - 1
            first.append(
                go(
                    remote(
                        modes_t.at[:, pl.ds(h * 1024, 1024)], cm.at[h, row],
                        m1s.at[n], m1r.at[n], r, col,
                    )
                )
            )
    def leg_a(n):
        r = at.row_at(*ROW_OFFS[n])
        go(remote(ma1.at[r], arr_ma.at[n], ma1s.at[n], ma1r.at[n], r, col))
        go(remote(a1.at[r], arr_a.at[n], a1s.at[n], a1r.at[n], r, col))

    def leg_b(n):
        c = at.col_at(*COL_OFFS[n])
        go(remote(mb1.at[pl.ds(2 * c, 2)], arr_mb.at[n], mb1s.at[n], mb1r.at[n], row, c))
        go(remote(b1.at[pl.ds(2 * c, 2)], arr_b.at[n], b1s.at[n], b1r.at[n], row, c))

    for n in range(1, 16):
        leg_a(n)
        if n < 8:
            leg_b(n)

    def wait_in(dst, rsem):
        remote(dst, dst, rsem, rsem, row, col).wait_recv()

    locals_[4].wait()
    locals_[5].wait()
    for d in (0, 1, 3, 2):
        for h in range(2):
            if d:
                back = at.row_at(4 - d, 0) if h == 0 else at.row_at(0, 4 - d)
                wait_in(cm.at[h, back], m1r.at[h * 3 + d - 1])
            else:
                back = row
            for e in (1, 3, 2):
                r = at.row_at(0, e) if h == 0 else at.row_at(e, 0)
                n = h * 12 + d * 3 + e - 1
                go(remote(cm.at[h, back], cm.at[h, back], m2s.at[n], m2r.at[n], r, col))

    lanes = lax.broadcasted_iota(I32, (8, BLK), 1)
    pk_ma[...] = jnp.zeros_like(pk_ma)
    pk_mb[...] = jnp.zeros_like(pk_mb)

    def pack_a(n, carry):
        meta = arr_ma[n]
        base = lax.rem(meta[4:5, :], 8) * 16 + 1
        for o in range(8):
            c = at.col_at(*COL_OFFS[o])
            total = jnp.zeros((BLK, BLK), BF16)
            slot = jnp.zeros((1, BLK), I32)
            for b in range(4):
                q = meta[b : b + 1, :]
                hit = lax.div(q, 16) == c
                mask = jnp.where(hit, F32(1.0), F32(0.0)).astype(BF16)
                total = total + arr_a[n, :, b * BLK : (b + 1) * BLK] * mask
                slot = slot + jnp.where(hit, base + lax.rem(q, 16), 0)
            pk_a[o, n] = total
            pk_ma[o] = pk_ma[o] + jnp.where(lanes == n, slot, 0)
        return carry

    def pack_b(n, carry):
        def each(o, inner):
            r = lax.rem(at.z + lax.div(o, 4), 4) * 4 + lax.rem(at.y + lax.rem(o, 4), 4)
            total = jnp.zeros((BLK, BLK), BF16)
            slot = jnp.zeros((1, BLK), I32)
            for h in range(2):
                meta = arr_mb[n, h]
                base = lax.rem(meta[4:5, :], 16) + 1
                for a in range(4):
                    p = meta[a : a + 1, :]
                    hit = lax.div(p, 8) == r
                    mask = jnp.where(hit, F32(1.0), F32(0.0)).astype(BF16)
                    total = total + arr_b[n, h, a * BLK : (a + 1) * BLK, :] * mask
                    slot = slot + jnp.where(hit, base + lax.rem(p, 8) * 16, 0)
            pk_b[o, n] = total
            pk_mb[o] = pk_mb[o] + jnp.where(lanes == n, slot, 0)
            return inner

        return lax.fori_loop(0, 16, each, carry)

    own_out = []

    def second_a(g):
        for n in range(4 * g, 4 * g + 4):
            if n:
                wait_in(arr_ma.at[n], ma1r.at[n])
                wait_in(arr_a.at[n], a1r.at[n])
        lax.fori_loop(4 * g, 4 * g + 4, pack_a, 0)
        for o in range(1, 8):
            c = at.col_at(*COL_OFFS[o])
            part = pl.ds(4 * g, 4)
            go(
                remote(
                    pk_a.at[o, part], a2.at[o, part],
                    a2s.at[o * 4 + g], a2r.at[o * 4 + g], row, c,
                )
            )
        keep = pltpu.make_async_copy(
            pk_a.at[0, pl.ds(4 * g, 4)], a2.at[0, pl.ds(4 * g, 4)], local.at[6 + g]
        )
        keep.start()
        own_out.append(keep)

    def second_b(g):
        for n in range(4 * g, 4 * g + 4):
            if n:
                wait_in(arr_mb.at[n], mb1r.at[n])
                wait_in(arr_b.at[n], b1r.at[n])
        lax.fori_loop(4 * g, 4 * g + 4, pack_b, 0)
        for o in range(1, 16):
            r = at.row_at(*ROW_OFFS[o])
            part = pl.ds(4 * g, 4)
            go(
                remote(
                    pk_b.at[o, part], b2.at[o, part],
                    b2s.at[o * 2 + g], b2r.at[o * 2 + g], r, col,
                )
            )
        keep = pltpu.make_async_copy(
            pk_b.at[0, pl.ds(4 * g, 4)], b2.at[0, pl.ds(4 * g, 4)], local.at[10 + g]
        )
        keep.start()
        own_out.append(keep)

    for copy in locals_[:4]:
        copy.wait()
    second_a(0)
    second_b(0)
    second_a(1)
    second_a(2)
    second_b(1)
    second_a(3)
    for o in range(1, 8):
        go(remote(pk_ma.at[o], ma2.at[o], ma2s.at[o], ma2r.at[o], row, at.col_at(*COL_OFFS[o])))
    for o in range(1, 16):
        go(remote(pk_mb.at[o], mb2.at[o], mb2s.at[o], mb2r.at[o], at.row_at(*ROW_OFFS[o]), col))
    for ref, out, n in ((pk_ma, ma2, 12), (pk_mb, mb2, 13)):
        keep = pltpu.make_async_copy(ref.at[0], out.at[0], local.at[n])
        keep.start()
        own_out.append(keep)

    for d in (0, 1, 3, 2):
        for h in range(2):
            for e in (1, 3, 2):
                if h == 0:
                    back = at.row_at(4 - d, 4 - e)
                else:
                    back = at.row_at(4 - e, 4 - d)
                n = h * 12 + d * 3 + e - 1
                wait_in(cm.at[h, back], m2r.at[n])
    lane = lax.div(at.y, 2)
    half = lax.rem(row, 2)
    on_lane = at.k == lane
    root = jnp.logical_and(on_lane, at.x == at.z)
    inner = jnp.logical_and(on_lane, at.x != at.z)
    far = (lax.rem(at.x + 4 - at.z, 4), lax.rem(at.z + 4 - at.x, 4))
    sibling = at.col_at(0, 1)

    def chain(n):
        step = at.col_at(1, 0) if n < 8 else at.col_at(3, 0)
        onward = remote(rm.at[n], rm.at[n], chs.at[n], chr_.at[n], row, step)
        across = remote(rm.at[n], rm.at[n], sbs.at[n], sbr.at[n], row, sibling)
        start = remote(cm.at[half, n], rm.at[n], chs.at[n], chr_.at[n], row, step)
        start_across = remote(cm.at[half, n], rm.at[n], sbs.at[n], sbr.at[n], row, sibling)
        forwards = jnp.logical_and(inner, far[0 if n < 8 else 1] < 3)
        return onward, across, start, start_across, forwards

    order = [n for pair in zip(range(8), range(8, 16)) for n in pair]
    for n in order:
        onward, across, start, start_across, forwards = chain(n)

        @pl.when(root)
        def _():
            start.start()
            start_across.start()

        @pl.when(inner)
        def _():
            onward.wait_recv()
            across.start()

        @pl.when(forwards)
        def _():
            onward.start()

    for n in order:
        onward, across, start, start_across, forwards = chain(n)

        @pl.when(on_lane)
        def _():
            across.wait_send()

        @pl.when(jnp.logical_not(on_lane))
        def _():
            across.wait_recv()

        @pl.when(jnp.logical_or(root, forwards))
        def _():
            onward.wait_send()

    for o in range(1, 8):
        for g in range(4):
            wait_in(a2.at[o, pl.ds(4 * g, 4)], a2r.at[o * 4 + g])
        wait_in(ma2.at[o], ma2r.at[o])
    for o in range(1, 16):
        for g in range(2):
            wait_in(b2.at[o, pl.ds(4 * g, 4)], b2r.at[o * 2 + g])
        wait_in(mb2.at[o], mb2r.at[o])
    for copy in own_out:
        copy.wait()
    for copy in sends:
        copy.wait_send()


def exchange(a1, b1, ma1, mb1, modes_t):
    edge = a1.shape[2]
    return pl.pallas_call(
        exchange_kernel,
        in_specs=[ANY] * 5,
        out_specs=[ANY] * 6,
        out_shape=[
            jax.ShapeDtypeStruct((8, 16, BLK, BLK), BF16),
            jax.ShapeDtypeStruct((16, 8, BLK, BLK), BF16),
            jax.ShapeDtypeStruct((8, 8, BLK), I32),
            jax.ShapeDtypeStruct((16, 8, BLK), I32),
            jax.ShapeDtypeStruct((2, 16, 64, 1024), BF16),
            jax.ShapeDtypeStruct((16, 64, 1024), BF16),
        ],
        scratch_shapes=[
            pltpu.VMEM((16, BLK, edge), BF16),
            pltpu.VMEM((8, 2, edge, BLK), BF16),
            pltpu.VMEM((16, 8, BLK), I32),
            pltpu.VMEM((8, 2, 8, BLK), I32),
            pltpu.VMEM((8, 16, BLK, BLK), BF16),
            pltpu.VMEM((16, 8, BLK, BLK), BF16),
            pltpu.VMEM((8, 8, BLK), I32),
            pltpu.VMEM((16, 8, BLK), I32),
            DMA((16,)), DMA((16,)), DMA((8,)), DMA((8,)),
            DMA((16,)), DMA((16,)), DMA((8,)), DMA((8,)),
            DMA((32,)), DMA((32,)), DMA((32,)), DMA((32,)),
            DMA((8,)), DMA((8,)), DMA((16,)), DMA((16,)),
            DMA((6,)), DMA((6,)), DMA((24,)), DMA((24,)),
            DMA((16,)), DMA((16,)), DMA((16,)), DMA((16,)),
            DMA((16,)),
        ],
        compiler_params=pltpu.CompilerParams(collective_id=0, has_side_effects=True),
        name="exchange",
    )(a1, b1, ma1, mb1, modes_t)


def assemble_kernel(
    a2, b2, ma2, mb2, cm, rm,
    stiff_out, mass_out, part_out, diag_out,
    va, vb, sa, sb, vcm, vrm, acc, tile, mass_tile, image, part, sems,
):
    at = Place()
    half = lax.rem(at.row, 2)
    holder = at.col == lax.div(at.row, 2)
    copies = [
        pltpu.make_async_copy(ma2, sa, sems.at[0]),
        pltpu.make_async_copy(a2, va, sems.at[1]),
        pltpu.make_async_copy(cm, vcm, sems.at[2]),
        pltpu.make_async_copy(mb2, sb, sems.at[3]),
        pltpu.make_async_copy(b2, vb, sems.at[4]),
    ]
    for copy in copies:
        copy.start()

    @pl.when(holder)
    def _():
        pltpu.make_async_copy(cm.at[half], vrm, sems.at[5]).start()

    @pl.when(jnp.logical_not(holder))
    def _():
        pltpu.make_async_copy(rm, vrm, sems.at[5]).start()

    def clear():
        def one(n, carry):
            acc[n] = jnp.zeros((BLK, BLK), F32)
            return carry

        lax.fori_loop(0, 128, one, 0)

    def gather(blocks, slots, senders, each):
        def one(n, carry):
            o, k = lax.div(n, each), lax.rem(n, each)
            slot = slots[o, 0, k]

            @pl.when(slot > 0)
            def _():
                acc[slot - 1] = acc[slot - 1] + blocks[o, k].astype(F32)

            return carry

        lax.fori_loop(0, senders * each, one, 0)

    def round_to(out):
        def one(p, carry):
            rows = pl.ds(pl.multiple_of(p * BLK, BLK), BLK)
            for q in range(16):
                out[rows, q * BLK : (q + 1) * BLK] = acc[p * 16 + q].astype(BF16)
            return carry

        lax.fori_loop(0, 8, one, 0)

    def products(source, offset):
        width = vcm.shape[3]
        for m in range(4):
            total = None
            for h in range(2):
                modes = vcm[h, 4 * m : 4 * m + 4].reshape(256, width)
                add = lax.dot_general(
                    source[:, h * width : (h + 1) * width], modes,
                    (((1,), (1,)), ((), ())), preferred_element_type=F32,
                )
                total = add if total is None else total + add
            image[...] = total.astype(BF16)
            left = vrm[...].reshape(1024, width)
            part[:, offset + m * 256 : offset + (m + 1) * 256] = jnp.dot(
                left, image[...], preferred_element_type=F32
            ).astype(BF16)

    clear()
    copies[0].wait()
    copies[1].wait()
    gather(va, sa, 8, 16)
    round_to(tile)
    out_stiff = pltpu.make_async_copy(tile, stiff_out, sems.at[6])
    out_stiff.start()
    copies[2].wait()
    pltpu.make_async_copy(rm, vrm, sems.at[5]).wait()
    products(tile, 0)
    out_first = pltpu.make_async_copy(
        part.at[:, pl.ds(0, 1024)], part_out.at[:, pl.ds(0, 1024)], sems.at[8]
    )
    out_first.start()
    clear()
    copies[3].wait()
    copies[4].wait()
    gather(vb, sb, 16, 8)
    round_to(mass_tile)
    out_stiff.wait()
    products(mass_tile, 1024)
    row_ids = lax.broadcasted_iota(I32, (BLK, BLK), 0)
    col_ids = lax.broadcasted_iota(I32, (BLK, BLK), 1)
    same = row_ids == col_ids

    @pl.when(holder)
    def _():
        for p in range(8):
            block = acc[p * 17 + half * 8]
            line = jnp.sum(jnp.where(same, block, F32(0.0)), axis=0, keepdims=True)
            diag_out[p] = jnp.broadcast_to(line, (8, BLK))
            rest = jnp.where(same, F32(0.0), block).astype(BF16)
            mass_tile[p * BLK : (p + 1) * BLK, pl.ds(pl.multiple_of(half * 1024 + p * BLK, BLK), BLK)] = rest

    @pl.when(jnp.logical_not(holder))
    def _():
        diag_out[...] = jnp.zeros_like(diag_out)

    out_mass = pltpu.make_async_copy(mass_tile, mass_out, sems.at[7])
    out_mass.start()
    out_second = pltpu.make_async_copy(
        part.at[:, pl.ds(1024, 1024)], part_out.at[:, pl.ds(1024, 1024)], sems.at[9]
    )
    out_second.start()
    out_first.wait()
    out_mass.wait()
    out_second.wait()


def assemble(a2, b2, ma2, mb2, cm, rm):
    return pl.pallas_call(
        assemble_kernel,
        in_specs=[ANY] * 6,
        out_specs=[ANY, ANY, ANY, VMEM],
        out_shape=[
            jax.ShapeDtypeStruct((1024, 2048), BF16),
            jax.ShapeDtypeStruct((1024, 2048), BF16),
            jax.ShapeDtypeStruct((1024, 2048), BF16),
            jax.ShapeDtypeStruct((8, 8, BLK), F32),
        ],
        scratch_shapes=[
            pltpu.VMEM((8, 16, BLK, BLK), BF16),
            pltpu.VMEM((16, 8, BLK, BLK), BF16),
            pltpu.SMEM((8, 8, BLK), I32),
            pltpu.SMEM((16, 8, BLK), I32),
            pltpu.VMEM((2, 16, 64, 1024), BF16),
            pltpu.VMEM((16, 64, 1024), BF16),
            pltpu.VMEM((128, BLK, BLK), F32),
            pltpu.VMEM((1024, 2048), BF16),
            pltpu.VMEM((1024, 2048), BF16),
            pltpu.VMEM((1024, 256), BF16),
            pltpu.VMEM((1024, 2048), BF16),
            DMA((10,)),
        ],
        compiler_params=pltpu.CompilerParams(vmem_limit_bytes=60 * 1024 * 1024),
        name="assemble",
    )(a2, b2, ma2, mb2, cm, rm)


def reduce_kernel(
    part, diag,
    stiff_out, mass_out, diag_out,
    own, other, sum_near, arr_row, sum_row, arr_x, send_last, arr_last,
    ns, nr, rs, rr, xs, xr, ls, lr, ds, dr, local,
):
    at = Place()
    row, col = at.row, at.col

    def remote(src, dst, ssem, rsem, r, c):
        return pltpu.make_async_remote_copy(
            src_ref=src, dst_ref=dst, send_sem=ssem, recv_sem=rsem,
            device_id=(r, c), device_id_type=MESH,
        )

    barrier = pltpu.get_barrier_semaphore()
    for dz, dy in ROW_OFFS[1:]:
        pl.semaphore_signal(barrier, inc=1, device_id=(at.row_at(dz, dy), col), device_id_type=MESH)
    for dx, dk in COL_OFFS[1:]:
        pl.semaphore_signal(barrier, inc=1, device_id=(row, at.col_at(dx, dk)), device_id_type=MESH)
    sibling = at.col_at(0, 1)
    mine = pl.ds(pl.multiple_of(at.k * 1024, 1024), 1024)
    theirs = pl.ds(pl.multiple_of((1 - at.k) * 1024, 1024), 1024)
    load = pltpu.make_async_copy(part.at[:, mine], own, local.at[0])
    load.start()
    pl.semaphore_wait(barrier, 22)
    near = remote(part.at[:, theirs], other, ns.at[0], nr.at[0], row, sibling)
    near.start()
    holder = col == lax.div(row, 2)

    def diag_copy(o):
        c = at.col_at(*COL_OFFS[o])
        return remote(diag.at[c], diag_out, ds.at[o], dr.at[0], row, c)

    @pl.when(holder)
    def _():
        for o in range(1, 8):
            diag_copy(o).start()
        keep = pltpu.make_async_copy(diag.at[col], diag_out, local.at[1])
        keep.start()
        keep.wait()

    load.wait()
    near.wait_recv()

    def add_near(n, carry):
        rows = pl.ds(pl.multiple_of(n * 64, 64), 64)
        sum_near[n] = (own[rows, :].astype(F32) + other[rows, :].astype(F32)).astype(BF16)
        return carry

    lax.fori_loop(0, 16, add_near, 0)
    row_sends = []
    for o in range(1, 16):
        r = at.row_at(*ROW_OFFS[o])
        copy = remote(sum_near.at[r], arr_row.at[o], rs.at[o], rr.at[o], r, col)
        copy.start()
        row_sends.append(copy)
    for copy in row_sends:
        copy.wait_recv()
    for n in range(4):
        lines = slice(n * 16, (n + 1) * 16)
        total = sum_near[row, lines, :].astype(F32)
        for o in range(1, 16):
            total = total + arr_row[o, lines, :].astype(F32)
        sum_row[n] = total.astype(BF16)
    x_sends = []
    for d in range(1, 4):
        xx = lax.rem(at.x + d, 4)
        copy = remote(
            sum_row.at[xx], arr_x.at[d], xs.at[d], xr.at[d], row, at.col_at(d, 0)
        )
        copy.start()
        x_sends.append(copy)
    for copy in x_sends:
        copy.wait_recv()
    total = sum_row[at.x].astype(F32)
    for d in range(1, 4):
        total = total + arr_x[d].astype(F32)
    send_last[0] = total[0:8, :]
    send_last[1] = total[8:16, :]
    last = remote(send_last.at[1 - at.k], arr_last, ls.at[0], lr.at[0], row, sibling)
    last.start()
    last.wait_recv()
    kept = send_last[at.k]
    got = arr_last[...]
    first = at.k == 0
    stiff_out[...] = jnp.where(first, kept, got)
    mass_out[...] = jnp.where(first, got, kept)

    @pl.when(jnp.logical_not(holder))
    def _():
        diag_copy(0).wait_recv()

    @pl.when(holder)
    def _():
        for o in range(1, 8):
            diag_copy(o).wait_send()

    near.wait_send()
    for copy in row_sends + x_sends + [last]:
        copy.wait_send()


def reduce_parts(part, diag):
    return pl.pallas_call(
        reduce_kernel,
        in_specs=[ANY, VMEM],
        out_specs=[VMEM, VMEM, VMEM],
        out_shape=[
            jax.ShapeDtypeStruct((8, 1024), F32),
            jax.ShapeDtypeStruct((8, 1024), F32),
            jax.ShapeDtypeStruct((8, BLK), F32),
        ],
        scratch_shapes=[
            pltpu.VMEM((1024, 1024), BF16),
            pltpu.VMEM((1024, 1024), BF16),
            pltpu.VMEM((16, 64, 1024), BF16),
            pltpu.VMEM((16, 64, 1024), BF16),
            pltpu.VMEM((4, 16, 1024), BF16),
            pltpu.VMEM((4, 16, 1024), BF16),
            pltpu.VMEM((2, 8, 1024), F32),
            pltpu.VMEM((8, 1024), F32),
            DMA((1,)), DMA((1,)), DMA((16,)), DMA((16,)), DMA((4,)), DMA((4,)),
            DMA((1,)), DMA((1,)), DMA((8,)), DMA((1,)), DMA((2,)),
        ],
        compiler_params=pltpu.CompilerParams(collective_id=1, has_side_effects=True),
        name="reduce",
    )(part, diag)


def body(inv_interior, coupling, boundary_stiff, mass_interior, mass_boundary, block_map, modes):
    a1, b1, ma1, mb1 = condense(
        inv_interior, coupling, boundary_stiff, mass_interior, mass_boundary, block_map
    )
    moved = exchange(a1, b1, ma1, mb1, modes.T)
    stiff_tile, mass_tile, part, diag = assemble(*moved)
    stiff, mass, diagonal = reduce_parts(part, diag)
    return stiff_tile, mass_tile, stiff, mass, diagonal[0]


def solution(mesh):
    both = ("row", "col")
    return jax.shard_map(
        body,
        mesh=mesh,
        in_specs=(
            P(both, None, None),
            P(both, None, None),
            P(both, None, None),
            P(both, None),
            P(both, None),
            P(both, None),
            P("col", "row"),
        ),
        out_specs=(
            P("row", "col"),
            P("row", "col"),
            P(both, None),
            P(both, None),
            P(both),
        ),
        check_vma=False,
    )
```

```python
import functools

import jax
import jax.numpy as jnp
from jax import lax
from jax.experimental import pallas as pl
from jax.experimental.pallas import tpu as pltpu
from jax.sharding import PartitionSpec as P

MESH = pl.DeviceIdType.MESH
BLK = 128
F32 = jnp.float32
BF16 = jnp.bfloat16
I32 = jnp.int32
ANY = pl.BlockSpec(memory_space=pl.ANY)
VMEM = pl.BlockSpec(memory_space=pltpu.VMEM)
DMA = pltpu.SemaphoreType.DMA
ROW_OFFS = [(dz, dy) for dz in range(4) for dy in range(4)]
COL_OFFS = [(dx, dk) for dx in range(4) for dk in range(2)]


class Place:
    def __init__(self):
        self.row = lax.axis_index("row")
        self.col = lax.axis_index("col")
        self.z, self.y = lax.div(self.row, 4), lax.rem(self.row, 4)
        self.x, self.k = lax.div(self.col, 2), lax.rem(self.col, 2)

    def row_at(self, dz, dy):
        return lax.rem(self.z + dz, 4) * 4 + lax.rem(self.y + dy, 4)

    def col_at(self, dx, dk):
        return lax.rem(self.x + dx, 4) * 2 + lax.rem(self.k + dk, 2)


THIRDS = ((0, 6), (6, 4), (10, 6))


def exchange_kernel(
    map_ref, inv, couple, stiff, mi_ref, mb_ref, modes_t,
    a2, b2, ma2, mb2, cm, rm,
    v_inv, v_couple, v_stiff, nat_a, nat_b, st_a, st_b, st_ma, st_mb,
    arr_a, arr_b, arr_ma, arr_mb, pk_a, pk_b, pk_ma, pk_mb,
    lds, a1s, a1r, b1s, b1r, ma1s, ma1r, mb1s, mb1r,
    a2s, a2r, b2s, b2r, ma2s, ma2r, mb2s, mb2r,
    m1s, m1r, m2s, m2r, rms, rmr, sbs, sbr, local,
):
    at = Place()
    row, col = at.row, at.col

    def remote(src, dst, ssem, rsem, r, c):
        return pltpu.make_async_remote_copy(
            src_ref=src, dst_ref=dst, send_sem=ssem, recv_sem=rsem,
            device_id=(r, c), device_id_type=MESH,
        )

    barrier = pltpu.get_barrier_semaphore()
    for dz, dy in ROW_OFFS[1:]:
        pl.semaphore_signal(barrier, inc=1, device_id=(at.row_at(dz, dy), col), device_id_type=MESH)
    for dx, dk in COL_OFFS[1:]:
        pl.semaphore_signal(barrier, inc=1, device_id=(row, at.col_at(dx, dk)), device_id_type=MESH)

    def loads(s):
        return [
            pltpu.make_async_copy(inv.at[s], v_inv.at[s], lds.at[0, s]),
            pltpu.make_async_copy(couple.at[s], v_couple.at[s], lds.at[1, s]),
            pltpu.make_async_copy(stiff.at[s], v_stiff.at[s], lds.at[2, s]),
        ]

    for s in range(4):
        for copy in loads(s):
            copy.start()
    own_modes = [
        pltpu.make_async_copy(modes_t.at[:, pl.ds(h * 1024, 1024)], cm.at[h, row], local.at[h])
        for h in range(2)
    ]
    for copy in own_modes:
        copy.start()

    sends = []

    def go(copy):
        copy.start()
        sends.append(copy)

    def wait_in(dst, rsem):
        remote(dst, dst, rsem, rsem, row, col).wait_recv()

    def condense(s, carry):
        for copy in loads(s):
            copy.wait()
        pair = v_couple[s]
        static = (-jnp.dot(v_inv[s], pair, preferred_element_type=F32)).astype(BF16)
        stiffness = v_stiff[s].astype(F32) + lax.dot_general(
            pair, static, (((0,), (0,)), ((), ())), preferred_element_type=F32
        )
        stiffness = stiffness.astype(BF16)
        for a in range(4):
            nat_a[s * 4 + a] = stiffness[a * BLK : (a + 1) * BLK, :]
        static_t = static.T
        weighted_t = (static_t.astype(F32) * mi_ref[pl.ds(s, 1), :]).astype(BF16)
        mass = lax.dot_general(
            static_t, weighted_t, (((1,), (1,)), ((), ())), preferred_element_type=F32
        )
        width = mass.shape[0]
        row_ids = lax.broadcasted_iota(I32, (width, width), 0)
        col_ids = lax.broadcasted_iota(I32, (width, width), 1)
        mass = mass + jnp.where(row_ids == col_ids, mb_ref[pl.ds(s, 1), :], F32(0.0))
        mass = mass.astype(BF16)
        for b in range(4):
            nat_b[s * 4 + b] = mass[:, b * BLK : (b + 1) * BLK]
        return carry

    lax.fori_loop(0, 1, condense, 0)
    pl.semaphore_wait(barrier, 22)
    for d in (1, 3, 2):
        for h in range(2):
            r = at.row_at(d, 0) if h == 0 else at.row_at(0, d)
            n = h * 3 + d - 1
            go(
                remote(
                    modes_t.at[:, pl.ds(h * 1024, 1024)], cm.at[h, row],
                    m1s.at[n], m1r.at[n], r, col,
                )
            )
    lax.fori_loop(1, 3, condense, 0)
    for copy in own_modes:
        copy.wait()
    for d in (0, 1, 3, 2):
        for h in range(2):
            if d:
                back = at.row_at(4 - d, 0) if h == 0 else at.row_at(0, 4 - d)
                wait_in(cm.at[h, back], m1r.at[h * 3 + d - 1])
            else:
                back = row
            for e in (1, 3, 2):
                r = at.row_at(0, e) if h == 0 else at.row_at(e, 0)
                n = h * 12 + d * 3 + e - 1
                go(remote(cm.at[h, back], cm.at[h, back], m2s.at[n], m2r.at[n], r, col))
    lax.fori_loop(3, 4, condense, 0)

    lines = lax.broadcasted_iota(I32, (8, BLK), 0)

    def find(tile_row):
        found = jnp.int32(0)
        for n in range(16):
            found = jnp.where(lax.div(map_ref[n // 4, n % 4], 8) == tile_row, n, found)
        sub = lax.div(found, 4)
        table = jnp.full((8, BLK), map_ref[sub, lax.rem(found, 4)], I32)
        for a in range(4):
            table = jnp.where(lines == a, map_ref[sub, a], table)
        return found, table

    def stage_a(o, carry):
        r = lax.rem(at.z + lax.div(o, 4), 4) * 4 + lax.rem(at.y + lax.rem(o, 4), 4)
        found, table = find(r)
        st_a[o] = nat_a[found]
        st_ma[o] = table
        return carry

    def stage_b(o, carry):
        n, h = lax.div(o, 2), lax.rem(o, 2)
        c = lax.rem(at.x + lax.div(n, 2), 4) * 2 + lax.rem(at.k + lax.rem(n, 2), 2)
        found, table = find(2 * c + h)
        st_b[n, h] = nat_b[found]
        st_mb[n, h] = table
        return carry

    lax.fori_loop(0, 16, stage_b, 0)
    for n in range(1, 8):
        c = at.col_at(*COL_OFFS[n])
        go(remote(st_mb.at[n], arr_mb.at[n], mb1s.at[n], mb1r.at[n], row, c))
        go(remote(st_b.at[n], arr_b.at[n], b1s.at[n], b1r.at[n], row, c))
    lax.fori_loop(0, 16, stage_a, 0)
    for n in range(1, 16):
        r = at.row_at(*ROW_OFFS[n])
        go(remote(st_ma.at[n], arr_ma.at[n], ma1s.at[n], ma1r.at[n], r, col))
        go(remote(st_a.at[n], arr_a.at[n], a1s.at[n], a1r.at[n], r, col))
    arr_a[0] = st_a[0]
    arr_ma[0] = st_ma[0]
    arr_b[0] = st_b[0]
    arr_mb[0] = st_mb[0]
    pk_ma[...] = jnp.zeros_like(pk_ma)
    pk_mb[...] = jnp.zeros_like(pk_mb)
    lanes = lax.broadcasted_iota(I32, (8, BLK), 1)

    for d in (0, 1, 3, 2):
        for h in range(2):
            for e in (1, 3, 2):
                back = at.row_at(4 - d, 4 - e) if h == 0 else at.row_at(4 - e, 4 - d)
                wait_in(cm.at[h, back], m2r.at[h * 12 + d * 3 + e - 1])
    half = lax.rem(row, 2)
    on_lane = at.k == lax.div(at.y, 2)
    place = lax.rem(at.x + 4 - at.z, 4)
    root = jnp.logical_and(on_lane, place == 0)
    inner = jnp.logical_and(on_lane, place > 0)
    sibling = at.col_at(0, 1)

    def third(t):
        return pl.ds(THIRDS[t][0], THIRDS[t][1])

    def out_third(t):
        return remote(
            cm.at[half, third(t)], rm.at[third(t)], rms.at[t], rmr.at[t], row, at.col_at(t + 1, 0)
        )

    def root_across(t):
        return remote(
            cm.at[half, third(t)], rm.at[third(t)], sbs.at[t], sbr.at[t], row, sibling
        )

    def across(t):
        return remote(rm.at[third(t)], rm.at[third(t)], sbs.at[t], sbr.at[t], row, sibling)

    def onward(t, u):
        return remote(
            rm.at[third(t)], rm.at[third(t)], rms.at[u], rmr.at[t], row, at.col_at(u + 4 - t, 0)
        )

    @pl.when(root)
    def _():
        for t in range(3):
            out_third(t).start()
            root_across(t).start()

    def pack_a(n, carry):
        meta = arr_ma[n]
        base = lax.rem(meta[4:5, :], 8) * 16 + 1
        for o in range(8):
            c = at.col_at(*COL_OFFS[o])
            total = jnp.zeros((BLK, BLK), BF16)
            slot = jnp.zeros((1, BLK), I32)
            for b in range(4):
                q = meta[b : b + 1, :]
                hit = lax.div(q, 16) == c
                mask = jnp.where(hit, F32(1.0), F32(0.0)).astype(BF16)
                total = total + arr_a[n, :, b * BLK : (b + 1) * BLK] * mask
                slot = jnp.where(hit, base + lax.rem(q, 16), slot)
            pk_a[o, n] = total
            pk_ma[o] = pk_ma[o] + jnp.where(lanes == n, slot, 0)
        return carry

    def pack_b(n, carry):
        def each(o, inside):
            r = lax.rem(at.z + lax.div(o, 4), 4) * 4 + lax.rem(at.y + lax.rem(o, 4), 4)
            total = jnp.zeros((BLK, BLK), BF16)
            slot = jnp.zeros((1, BLK), I32)
            for h in range(2):
                meta = arr_mb[n, h]
                base = lax.rem(meta[4:5, :], 16) + 1
                for a in range(4):
                    p = meta[a : a + 1, :]
                    hit = lax.div(p, 8) == r
                    mask = jnp.where(hit, F32(1.0), F32(0.0)).astype(BF16)
                    total = total + arr_b[n, h, a * BLK : (a + 1) * BLK, :] * mask
                    slot = jnp.where(hit, base + lax.rem(p, 8) * 16, slot)
            pk_b[o, n] = total
            pk_mb[o] = pk_mb[o] + jnp.where(lanes == n, slot, 0)
            return inside

        return lax.fori_loop(0, 16, each, carry)

    own_out = []

    def keep(src, dst, n):
        copy = pltpu.make_async_copy(src, dst, local.at[n])
        copy.start()
        own_out.append(copy)

    def second_a(g):
        part = pl.ds(4 * g, 4)
        for n in range(4 * g, 4 * g + 4):
            if n:
                wait_in(arr_ma.at[n], ma1r.at[n])
                wait_in(arr_a.at[n], a1r.at[n])
        lax.fori_loop(4 * g, 4 * g + 4, pack_a, 0)
        for o in range(1, 8):
            n = o * 4 + g
            go(
                remote(
                    pk_a.at[o, part], a2.at[o, part], a2s.at[n], a2r.at[n],
                    row, at.col_at(*COL_OFFS[o]),
                )
            )
        keep(pk_a.at[0, part], a2.at[0, part], 2 + g)

    def second_b(g):
        part = pl.ds(4 * g, 4)
        for n in range(4 * g, 4 * g + 4):
            if n:
                wait_in(arr_mb.at[n], mb1r.at[n])
                wait_in(arr_b.at[n], b1r.at[n])
        lax.fori_loop(4 * g, 4 * g + 4, pack_b, 0)
        for o in range(1, 16):
            n = o * 2 + g
            go(
                remote(
                    pk_b.at[o, part], b2.at[o, part], b2s.at[n], b2r.at[n],
                    at.row_at(*ROW_OFFS[o]), col,
                )
            )
        keep(pk_b.at[0, part], b2.at[0, part], 6 + g)

    second_a(0)
    second_b(0)
    second_a(1)
    second_b(1)
    for o in range(1, 16):
        go(remote(pk_mb.at[o], mb2.at[o], mb2s.at[o], mb2r.at[o], at.row_at(*ROW_OFFS[o]), col))
    for t in range(3):

        @pl.when(jnp.logical_and(inner, place == t + 1))
        def _():
            wait_in(rm.at[third(t)], rmr.at[t])
            for u in range(3):
                if u != t:
                    onward(t, u).start()
            across(t).start()

    second_a(2)
    second_a(3)
    for o in range(1, 8):
        go(remote(pk_ma.at[o], ma2.at[o], ma2s.at[o], ma2r.at[o], row, at.col_at(*COL_OFFS[o])))
    keep(pk_ma.at[0], ma2.at[0], 8)
    keep(pk_mb.at[0], mb2.at[0], 9)
    for t in range(3):

        @pl.when(jnp.logical_and(inner, place != t + 1))
        def _():
            wait_in(rm.at[third(t)], rmr.at[t])
            across(t).start()

    for o in range(1, 8):
        for g in range(4):
            wait_in(a2.at[o, pl.ds(4 * g, 4)], a2r.at[o * 4 + g])
        wait_in(ma2.at[o], ma2r.at[o])
    for o in range(1, 16):
        for g in range(2):
            wait_in(b2.at[o, pl.ds(4 * g, 4)], b2r.at[o * 2 + g])
        wait_in(mb2.at[o], mb2r.at[o])
    for copy in own_out:
        copy.wait()
    for t in range(3):

        @pl.when(root)
        def _():
            out_third(t).wait_send()

        @pl.when(on_lane)
        def _():
            across(t).wait_send()

        @pl.when(jnp.logical_not(on_lane))
        def _():
            across(t).wait_recv()

        @pl.when(jnp.logical_and(inner, place == t + 1))
        def _():
            for u in range(3):
                if u != t:
                    onward(t, u).wait_send()

    for copy in sends:
        copy.wait_send()


def exchange(block_map, inv_interior, coupling, boundary_stiff, mass_interior, mass_boundary, modes_t):
    subs, inside, edge = coupling.shape
    return pl.pallas_call(
        exchange_kernel,
        in_specs=[pl.BlockSpec(memory_space=pltpu.SMEM), ANY, ANY, ANY, VMEM, VMEM, ANY],
        out_specs=[ANY] * 6,
        out_shape=[
            jax.ShapeDtypeStruct((8, 16, BLK, BLK), BF16),
            jax.ShapeDtypeStruct((16, 8, BLK, BLK), BF16),
            jax.ShapeDtypeStruct((8, 8, BLK), I32),
            jax.ShapeDtypeStruct((16, 8, BLK), I32),
            jax.ShapeDtypeStruct((2, 16, 64, 1024), BF16),
            jax.ShapeDtypeStruct((16, 64, 1024), BF16),
        ],
        scratch_shapes=[
            pltpu.VMEM((subs, inside, inside), BF16),
            pltpu.VMEM((subs, inside, edge), BF16),
            pltpu.VMEM((subs, edge, edge), BF16),
            pltpu.VMEM((16, BLK, edge), BF16),
            pltpu.VMEM((16, edge, BLK), BF16),
            pltpu.VMEM((16, BLK, edge), BF16),
            pltpu.VMEM((8, 2, edge, BLK), BF16),
            pltpu.VMEM((16, 8, BLK), I32),
            pltpu.VMEM((8, 2, 8, BLK), I32),
            pltpu.VMEM((16, BLK, edge), BF16),
            pltpu.VMEM((8, 2, edge, BLK), BF16),
            pltpu.VMEM((16, 8, BLK), I32),
            pltpu.VMEM((8, 2, 8, BLK), I32),
            pltpu.VMEM((8, 16, BLK, BLK), BF16),
            pltpu.VMEM((16, 8, BLK, BLK), BF16),
            pltpu.VMEM((8, 8, BLK), I32),
            pltpu.VMEM((16, 8, BLK), I32),
            DMA((3, 4)),
            DMA((16,)), DMA((16,)), DMA((8,)), DMA((8,)),
            DMA((16,)), DMA((16,)), DMA((8,)), DMA((8,)),
            DMA((32,)), DMA((32,)), DMA((32,)), DMA((32,)),
            DMA((8,)), DMA((8,)), DMA((16,)), DMA((16,)),
            DMA((6,)), DMA((6,)), DMA((24,)), DMA((24,)),
            DMA((3,)), DMA((3,)), DMA((3,)), DMA((3,)),
            DMA((10,)),
        ],
        compiler_params=pltpu.CompilerParams(
            collective_id=0, has_side_effects=True, vmem_limit_bytes=60 * 1024 * 1024
        ),
        name="exchange",
    )(block_map, inv_interior, coupling, boundary_stiff, mass_interior, mass_boundary, modes_t)


def assemble_kernel(
    a2, b2, ma2, mb2,
    stiff_out, mass_out, diag_out,
    va, vb, sa, sb, acc, tile, mass_tile, sems,
):
    at = Place()
    half = lax.rem(at.row, 2)
    holder = at.col == lax.div(at.row, 2)
    copies = [
        pltpu.make_async_copy(ma2, sa, sems.at[0]),
        pltpu.make_async_copy(a2, va, sems.at[1]),
        pltpu.make_async_copy(mb2, sb, sems.at[2]),
        pltpu.make_async_copy(b2, vb, sems.at[3]),
    ]
    for copy in copies:
        copy.start()

    def clear(n, carry):
        acc[n] = jnp.zeros((BLK, BLK), F32)
        return carry

    def gather(base, blocks, slots, senders, each):
        def one(n, carry):
            for u in range(4):
                o, k = lax.div(n * 4, each), lax.rem(n * 4, each) + u
                slot = slots[o, 0, k] + base
                acc[slot] = acc[slot] + blocks[o, k].astype(F32)
            return carry

        lax.fori_loop(0, senders * each // 4, one, 0)

    def round_to(base, out):
        def one(p, carry):
            rows = pl.ds(pl.multiple_of(p * BLK, BLK), BLK)
            for q in range(16):
                out[rows, q * BLK : (q + 1) * BLK] = acc[base + p * 16 + q + 1].astype(BF16)
            return carry

        lax.fori_loop(0, 8, one, 0)

    lax.fori_loop(0, 258, clear, 0)
    copies[0].wait()
    copies[1].wait()
    gather(0, va, sa, 8, 16)
    round_to(0, tile)
    out_stiff = pltpu.make_async_copy(tile, stiff_out, sems.at[4])
    out_stiff.start()
    copies[2].wait()
    copies[3].wait()
    gather(129, vb, sb, 16, 8)
    round_to(129, mass_tile)
    row_ids = lax.broadcasted_iota(I32, (BLK, BLK), 0)
    col_ids = lax.broadcasted_iota(I32, (BLK, BLK), 1)
    same = row_ids == col_ids

    @pl.when(holder)
    def _():
        for p in range(8):
            block = acc[130 + p * 17 + half * 8]
            line = jnp.sum(jnp.where(same, block, F32(0.0)), axis=0, keepdims=True)
            diag_out[p] = jnp.broadcast_to(line, (8, BLK))
            rest = jnp.where(same, F32(0.0), block).astype(BF16)
            start = pl.multiple_of(half * 1024 + p * BLK, BLK)
            mass_tile[p * BLK : (p + 1) * BLK, pl.ds(start, BLK)] = rest

    @pl.when(jnp.logical_not(holder))
    def _():
        diag_out[...] = jnp.zeros_like(diag_out)

    out_mass = pltpu.make_async_copy(mass_tile, mass_out, sems.at[5])
    out_mass.start()
    out_stiff.wait()
    out_mass.wait()


def assemble(a2, b2, ma2, mb2):
    return pl.pallas_call(
        assemble_kernel,
        in_specs=[ANY] * 4,
        out_specs=[ANY, ANY, VMEM],
        out_shape=[
            jax.ShapeDtypeStruct((1024, 2048), BF16),
            jax.ShapeDtypeStruct((1024, 2048), BF16),
            jax.ShapeDtypeStruct((8, 8, BLK), F32),
        ],
        scratch_shapes=[
            pltpu.VMEM((8, 16, BLK, BLK), BF16),
            pltpu.VMEM((16, 8, BLK, BLK), BF16),
            pltpu.SMEM((8, 8, BLK), I32),
            pltpu.SMEM((16, 8, BLK), I32),
            pltpu.VMEM((258, BLK, BLK), F32),
            pltpu.VMEM((1024, 2048), BF16),
            pltpu.VMEM((1024, 2048), BF16),
            DMA((6,)),
        ],
        compiler_params=pltpu.CompilerParams(vmem_limit_bytes=60 * 1024 * 1024),
        name="assemble",
    )(a2, b2, ma2, mb2)


GROUPS = ((0, 6, "zyx"), (6, 6, "yxz"), (12, 4, "xzy"))


def reduce_kernel(
    stiff, mass, diag, cm, rm,
    stiff_out, mass_out, diag_out,
    tiles, vcm, vrm, *rest,
):
    bufs = [rest[7 * j : 7 * j + 7] for j in range(3)]
    send_last, arr_last = rest[21:23]
    ns, nr, s1, r1, s2, r2, s3, r3, ls, lr, ds, dr, local = rest[23:]
    at = Place()
    row, col = at.row, at.col
    half = lax.rem(row, 2)
    holder = col == lax.div(row, 2)
    mine = {"z": at.z, "y": at.y, "x": at.x}

    def remote(src, dst, ssem, rsem, r, c):
        return pltpu.make_async_remote_copy(
            src_ref=src, dst_ref=dst, send_sem=ssem, recv_sem=rsem,
            device_id=(r, c), device_id_type=MESH,
        )

    def away(axis, d):
        r = at.row_at(d if axis == "z" else 0, d if axis == "y" else 0)
        c = at.col_at(d if axis == "x" else 0, 0)
        return r, c, lax.rem(mine[axis] + d, 4)

    barrier = pltpu.get_barrier_semaphore()
    for d in range(1, 4):
        for axis in "zy":
            r, c, _ = away(axis, d)
            pl.semaphore_signal(barrier, inc=1, device_id=(r, c), device_id_type=MESH)
    for dx, dk in COL_OFFS[1:]:
        pl.semaphore_signal(barrier, inc=1, device_id=(row, at.col_at(dx, dk)), device_id_type=MESH)
    sibling = at.col_at(0, 1)
    loads = [
        pltpu.make_async_copy(cm, vcm, local.at[0]),
        pltpu.make_async_copy(stiff, tiles.at[0], local.at[1]),
        pltpu.make_async_copy(mass, tiles.at[1], local.at[2]),
    ]
    for copy in loads:
        copy.start()

    @pl.when(holder)
    def _():
        pltpu.make_async_copy(cm.at[half], vrm, local.at[3]).start()

    @pl.when(jnp.logical_not(holder))
    def _():
        pltpu.make_async_copy(rm, vrm, local.at[3]).start()

    for copy in loads:
        copy.wait()
    pltpu.make_async_copy(rm, vrm, local.at[3]).wait()

    @pl.when(holder)
    def _():
        row_ids = lax.broadcasted_iota(I32, (BLK, BLK), 0)
        col_ids = lax.broadcasted_iota(I32, (BLK, BLK), 1)
        for p in range(8):
            spot = (
                1,
                slice(p * BLK, (p + 1) * BLK),
                pl.ds(pl.multiple_of(half * 1024 + p * BLK, BLK), BLK),
            )
            block = tiles[spot].astype(F32)
            tiles[spot] = jnp.where(row_ids == col_ids, diag[p, 0:1, :], block).astype(BF16)

    pl.semaphore_wait(barrier, 13)

    def diag_copy(o):
        c = at.col_at(*COL_OFFS[o])
        return remote(diag.at[c], diag_out, ds.at[o], dr.at[0], row, c)

    @pl.when(holder)
    def _():
        for o in range(1, 8):
            diag_copy(o).start()
        own = pltpu.make_async_copy(diag.at[col], diag_out, local.at[4])
        own.start()
        own.wait()

    def product(which, j):
        first, count, _ = GROUPS[j]
        depth = vcm.shape[3]
        total = None
        for h in range(2):
            modes = vcm[h, first : first + count].reshape(count * 64, depth)
            add = lax.dot_general(
                tiles[which, :, h * depth : (h + 1) * depth], modes,
                (((1,), (1,)), ((), ())), preferred_element_type=F32,
            )
            total = add if total is None else total + add
        left = vrm[...].reshape(1024, depth)
        return jnp.dot(left, total.astype(BF16), preferred_element_type=F32)

    near = []
    for j in range(3):
        out_near, in_near = bufs[j][0], bufs[j][1]
        out_near[...] = product(1 - at.k, j).astype(BF16)
        copy = remote(out_near, in_near, ns.at[j], nr.at[j], row, sibling)
        copy.start()
        near.append(copy)
    sends = []

    def leg(j, level, src, dst, ssem, rsem):
        axis = GROUPS[j][2][level]
        dims = sorted(GROUPS[j][2][level:], key="zyx".index)
        spot = dims.index(axis)
        arriving = []
        for d in range(1, 4):
            r, c, place = away(axis, d)
            part = src.at[(slice(None),) * spot + (place,)]
            copy = remote(part, dst.at[d], ssem.at[j * 4 + d], rsem.at[j * 4 + d], r, c)
            copy.start()
            sends.append(copy)
            arriving.append(copy)
        return arriving, (slice(None),) * spot + (mine[axis],)

    def summed(src, own, dst, arriving):
        for copy in arriving:
            copy.wait_recv()
        total = src[own].astype(F32)
        for d in range(1, 4):
            total = total + dst[d].astype(F32)
        return total

    first_legs = []
    for j in range(3):
        _, in_near, near_sum, arr1, _, _, _ = bufs[j]
        width = GROUPS[j][1] * 64
        here = product(at.k, j)
        near[j].wait_recv()
        total = (here + in_near[...].astype(F32)).astype(BF16)
        near_sum[...] = total.reshape(4, 4, 4, 16, width)
        first_legs.append(leg(j, 0, near_sum, arr1, s1, r1))
    second_legs = []
    for j in range(3):
        _, _, near_sum, arr1, sum1, arr2, _ = bufs[j]
        arriving, own = first_legs[j]
        sum1[...] = summed(near_sum, own, arr1, arriving).astype(BF16)
        second_legs.append(leg(j, 1, sum1, arr2, s2, r2))
    third_legs = []
    for j in range(3):
        sum1, arr2, last = bufs[j][4:]
        arriving, own = second_legs[j]
        last[0] = summed(sum1, own, arr2, arriving).astype(BF16)
        third_legs.append(leg(j, 2, last.at[0], last.at[1], s3, r3))
    for j in range(3):
        last = bufs[j][6]
        arriving, own = third_legs[j]
        total = summed(last.at[0], own, last.at[1], arriving)
        cols = slice(GROUPS[j][0] * 64, (GROUPS[j][0] + GROUPS[j][1]) * 64)
        send_last[0, :, cols] = total[0:8, :]
        send_last[1, :, cols] = total[8:16, :]
    final = remote(send_last.at[1 - at.k], arr_last, ls.at[0], lr.at[0], row, sibling)
    final.start()
    final.wait_recv()
    kept = send_last[at.k]
    got = arr_last[...]
    lower = at.k == 0
    stiff_out[...] = jnp.where(lower, kept, got)
    mass_out[...] = jnp.where(lower, got, kept)

    @pl.when(jnp.logical_not(holder))
    def _():
        diag_copy(0).wait_recv()

    @pl.when(holder)
    def _():
        for o in range(1, 8):
            diag_copy(o).wait_send()

    for copy in near + sends + [final]:
        copy.wait_send()


def reduce_parts(stiff, mass, diag, cm, rm):
    scratch = [
        pltpu.VMEM((2, 1024, 2048), BF16),
        pltpu.VMEM((2, 16, 64, 1024), BF16),
        pltpu.VMEM((16, 64, 1024), BF16),
    ]
    for _, count, _ in GROUPS:
        width = count * 64
        scratch += [
            pltpu.VMEM((1024, width), BF16),
            pltpu.VMEM((1024, width), BF16),
            pltpu.VMEM((4, 4, 4, 16, width), BF16),
            pltpu.VMEM((4, 4, 4, 16, width), BF16),
            pltpu.VMEM((4, 4, 16, width), BF16),
            pltpu.VMEM((4, 4, 16, width), BF16),
            pltpu.VMEM((2, 4, 16, width), BF16),
        ]
    return pl.pallas_call(
        reduce_kernel,
        in_specs=[ANY, ANY, VMEM, ANY, ANY],
        out_specs=[VMEM, VMEM, VMEM],
        out_shape=[
            jax.ShapeDtypeStruct((8, 1024), F32),
            jax.ShapeDtypeStruct((8, 1024), F32),
            jax.ShapeDtypeStruct((8, BLK), F32),
        ],
        scratch_shapes=scratch
        + [
            pltpu.VMEM((2, 8, 1024), F32),
            pltpu.VMEM((8, 1024), F32),
            DMA((3,)), DMA((3,)),
            DMA((12,)), DMA((12,)), DMA((12,)), DMA((12,)), DMA((12,)), DMA((12,)),
            DMA((1,)), DMA((1,)), DMA((8,)), DMA((1,)), DMA((5,)),
        ],
        compiler_params=pltpu.CompilerParams(
            collective_id=1, has_side_effects=True, vmem_limit_bytes=60 * 1024 * 1024
        ),
        name="reduce",
    )(stiff, mass, diag, cm, rm)


def body(inv_interior, coupling, boundary_stiff, mass_interior, mass_boundary, block_map, modes):
    a2, b2, ma2, mb2, cm, rm = exchange(
        block_map, inv_interior, coupling, boundary_stiff, mass_interior, mass_boundary, modes.T
    )
    stiff_tile, mass_tile, diag = assemble(a2, b2, ma2, mb2)
    stiff, mass, diagonal = reduce_parts(stiff_tile, mass_tile, diag, cm, rm)
    return stiff_tile, mass_tile, stiff, mass, diagonal[0]


def solution(mesh):
    both = ("row", "col")
    return jax.shard_map(
        body,
        mesh=mesh,
        in_specs=(
            P(both, None, None),
            P(both, None, None),
            P(both, None, None),
            P(both, None),
            P(both, None),
            P(both, None),
            P("col", "row"),
        ),
        out_specs=(
            P("row", "col"),
            P("row", "col"),
            P(both, None),
            P(both, None),
            P(both),
        ),
        check_vma=False,
    )
```

```python
import functools

import jax
import jax.numpy as jnp
from jax import lax
from jax.experimental import pallas as pl
from jax.experimental.pallas import tpu as pltpu
from jax.sharding import PartitionSpec as P

MESH = pl.DeviceIdType.MESH
BLK = 128
LIFT = 32
REST = BLK - LIFT
F32 = jnp.float32
BF16 = jnp.bfloat16
I32 = jnp.int32
ANY = pl.BlockSpec(memory_space=pl.ANY)
VMEM = pl.BlockSpec(memory_space=pltpu.VMEM)
DMA = pltpu.SemaphoreType.DMA
ROW_OFFS = [(dz, dy) for dz in range(4) for dy in range(4)]
COL_OFFS = [(dx, dk) for dx in range(4) for dk in range(2)]


class Place:
    def __init__(self):
        self.row = lax.axis_index("row")
        self.col = lax.axis_index("col")
        self.z, self.y = lax.div(self.row, 4), lax.rem(self.row, 4)
        self.x, self.k = lax.div(self.col, 2), lax.rem(self.col, 2)

    def row_at(self, dz, dy):
        return lax.rem(self.z + dz, 4) * 4 + lax.rem(self.y + dy, 4)

    def col_at(self, dx, dk):
        return lax.rem(self.x + dx, 4) * 2 + lax.rem(self.k + dk, 2)


THIRDS = ((0, 6), (6, 4), (10, 6))


def exchange_kernel(
    map_ref, inv, couple, stiff, mi_ref, mb_ref, modes_t,
    a2, b2, ma2, mb2, cm, rm,
    v_inv, v_couple, v_stiff, nat_a, nat_b, st_a, st_b, st_ma, st_mb,
    arr_a, arr_b, arr_ma, arr_mb, pk_a, pk_b, pk_ma, pk_mb,
    lds, a1s, a1r, b1s, b1r, ma1s, ma1r, mb1s, mb1r,
    a2s, a2r, b2s, b2r, ma2s, ma2r, mb2s, mb2r,
    m1s, m1r, m2s, m2r, rms, rmr, sbs, sbr, local,
):
    at = Place()
    row, col = at.row, at.col

    def remote(src, dst, ssem, rsem, r, c):
        return pltpu.make_async_remote_copy(
            src_ref=src, dst_ref=dst, send_sem=ssem, recv_sem=rsem,
            device_id=(r, c), device_id_type=MESH,
        )

    barrier = pltpu.get_barrier_semaphore()
    for dz, dy in ROW_OFFS[1:]:
        pl.semaphore_signal(barrier, inc=1, device_id=(at.row_at(dz, dy), col), device_id_type=MESH)
    for dx, dk in COL_OFFS[1:]:
        pl.semaphore_signal(barrier, inc=1, device_id=(row, at.col_at(dx, dk)), device_id_type=MESH)

    def loads(s):
        return [
            pltpu.make_async_copy(inv.at[s], v_inv.at[s], lds.at[0, s]),
            pltpu.make_async_copy(couple.at[s], v_couple.at[s], lds.at[1, s]),
            pltpu.make_async_copy(stiff.at[s], v_stiff.at[s], lds.at[2, s]),
        ]

    for s in range(4):
        for copy in loads(s):
            copy.start()
    own_modes = [
        pltpu.make_async_copy(modes_t.at[:, pl.ds(h * 1024, 1024)], cm.at[h, row], local.at[h])
        for h in range(2)
    ]
    for copy in own_modes:
        copy.start()

    sends = []

    def go(copy):
        copy.start()
        sends.append(copy)

    def wait_in(dst, rsem):
        remote(dst, dst, rsem, rsem, row, col).wait_recv()

    def condense(s, carry):
        for copy in loads(s):
            copy.wait()
        pair = v_couple[s]
        static = (-jnp.dot(v_inv[s], pair, preferred_element_type=F32)).astype(BF16)
        stiffness = v_stiff[s].astype(F32) + lax.dot_general(
            pair, static, (((0,), (0,)), ((), ())), preferred_element_type=F32
        )
        stiffness = stiffness.astype(BF16)
        for a in range(4):
            nat_a[s * 4 + a, 0:BLK, :] = stiffness[a * BLK : (a + 1) * BLK, :]
        static_t = static.T
        weighted_t = (static_t.astype(F32) * mi_ref[pl.ds(s, 1), :]).astype(BF16)
        mass = lax.dot_general(
            static_t, weighted_t, (((1,), (1,)), ((), ())), preferred_element_type=F32
        )
        width = mass.shape[0]
        row_ids = lax.broadcasted_iota(I32, (width, width), 0)
        col_ids = lax.broadcasted_iota(I32, (width, width), 1)
        mass = mass + jnp.where(row_ids == col_ids, mb_ref[pl.ds(s, 1), :], F32(0.0))
        mass = mass.astype(BF16)
        for a in range(4):
            lifted = a * BLK + LIFT
            nat_a[s * 4 + a, BLK : BLK + LIFT, :] = mass[a * BLK : lifted, :]
            for b in range(4):
                nat_b[s * 4 + b, a * REST : (a + 1) * REST, :] = mass[
                    lifted : (a + 1) * BLK, b * BLK : (b + 1) * BLK
                ]
        return carry

    pl.semaphore_wait(barrier, 22)
    for d in (1, 3, 2):
        for h in range(2):
            r = at.row_at(d, 0) if h == 0 else at.row_at(0, d)
            n = h * 3 + d - 1
            go(
                remote(
                    modes_t.at[:, pl.ds(h * 1024, 1024)], cm.at[h, row],
                    m1s.at[n], m1r.at[n], r, col,
                )
            )
    lax.fori_loop(0, 2, condense, 0)
    for copy in own_modes:
        copy.wait()
    for d in (0, 1, 3, 2):
        for h in range(2):
            if d:
                back = at.row_at(4 - d, 0) if h == 0 else at.row_at(0, 4 - d)
                wait_in(cm.at[h, back], m1r.at[h * 3 + d - 1])
            else:
                back = row
            for e in (1, 3, 2):
                r = at.row_at(0, e) if h == 0 else at.row_at(e, 0)
                n = h * 12 + d * 3 + e - 1
                go(remote(cm.at[h, back], cm.at[h, back], m2s.at[n], m2r.at[n], r, col))
    lax.fori_loop(2, 4, condense, 0)

    lines = lax.broadcasted_iota(I32, (8, BLK), 0)

    def find(tile_row):
        found = jnp.int32(0)
        for n in range(16):
            found = jnp.where(lax.div(map_ref[n // 4, n % 4], 8) == tile_row, n, found)
        sub = lax.div(found, 4)
        table = jnp.full((8, BLK), map_ref[sub, lax.rem(found, 4)], I32)
        for a in range(4):
            table = jnp.where(lines == a, map_ref[sub, a], table)
        return found, table

    def stage_a(o, carry):
        r = lax.rem(at.z + lax.div(o, 4), 4) * 4 + lax.rem(at.y + lax.rem(o, 4), 4)
        found, table = find(r)
        st_a[o] = nat_a[found]
        st_ma[o] = table
        return carry

    def stage_b(o, carry):
        n, h = lax.div(o, 2), lax.rem(o, 2)
        c = lax.rem(at.x + lax.div(n, 2), 4) * 2 + lax.rem(at.k + lax.rem(n, 2), 2)
        found, table = find(2 * c + h)
        st_b[n, h] = nat_b[found]
        st_mb[n, h] = table
        return carry

    lax.fori_loop(0, 16, stage_b, 0)
    for n in range(1, 8):
        c = at.col_at(*COL_OFFS[n])
        go(remote(st_mb.at[n], arr_mb.at[n], mb1s.at[n], mb1r.at[n], row, c))
        go(remote(st_b.at[n], arr_b.at[n], b1s.at[n], b1r.at[n], row, c))
    lax.fori_loop(0, 16, stage_a, 0)
    for n in range(1, 16):
        r = at.row_at(*ROW_OFFS[n])
        go(remote(st_ma.at[n], arr_ma.at[n], ma1s.at[n], ma1r.at[n], r, col))
        go(remote(st_a.at[n], arr_a.at[n], a1s.at[n], a1r.at[n], r, col))
    arr_a[0] = st_a[0]
    arr_ma[0] = st_ma[0]
    arr_b[0] = st_b[0]
    arr_mb[0] = st_mb[0]
    pk_ma[...] = jnp.zeros_like(pk_ma)
    pk_mb[...] = jnp.zeros_like(pk_mb)
    lanes = lax.broadcasted_iota(I32, (8, BLK), 1)

    for d in (0, 1, 3, 2):
        for h in range(2):
            for e in (1, 3, 2):
                back = at.row_at(4 - d, 4 - e) if h == 0 else at.row_at(4 - e, 4 - d)
                wait_in(cm.at[h, back], m2r.at[h * 12 + d * 3 + e - 1])
    half = lax.rem(row, 2)
    on_lane = at.k == lax.div(at.y, 2)
    place = lax.rem(at.x + 4 - at.z, 4)
    root = jnp.logical_and(on_lane, place == 0)
    inner = jnp.logical_and(on_lane, place > 0)
    sibling = at.col_at(0, 1)

    def third(t):
        return pl.ds(THIRDS[t][0], THIRDS[t][1])

    def out_third(t):
        return remote(
            cm.at[half, third(t)], rm.at[third(t)], rms.at[t], rmr.at[t], row, at.col_at(t + 1, 0)
        )

    def root_across(t):
        return remote(
            cm.at[half, third(t)], rm.at[third(t)], sbs.at[t], sbr.at[t], row, sibling
        )

    def across(t):
        return remote(rm.at[third(t)], rm.at[third(t)], sbs.at[t], sbr.at[t], row, sibling)

    def onward(t, u):
        return remote(
            rm.at[third(t)], rm.at[third(t)], rms.at[u], rmr.at[t], row, at.col_at(u + 4 - t, 0)
        )

    @pl.when(root)
    def _():
        for t in range(3):
            out_third(t).start()
            root_across(t).start()

    def pack_a(n, carry):
        meta = arr_ma[n]
        base = lax.rem(meta[4:5, :], 8) * 16 + 1
        for o in range(8):
            c = at.col_at(*COL_OFFS[o])
            total = jnp.zeros((BLK + LIFT, BLK), BF16)
            slot = jnp.zeros((1, BLK), I32)
            for b in range(4):
                q = meta[b : b + 1, :]
                hit = lax.div(q, 16) == c
                mask = jnp.where(hit, F32(1.0), F32(0.0)).astype(BF16)
                total = total + arr_a[n, :, b * BLK : (b + 1) * BLK] * mask
                slot = jnp.where(hit, base + lax.rem(q, 16), slot)
            pk_a[o, n] = total
            pk_ma[o] = pk_ma[o] + jnp.where(lanes == n, slot, 0)
        return carry

    def pack_b(n, carry):
        def each(o, inside):
            r = lax.rem(at.z + lax.div(o, 4), 4) * 4 + lax.rem(at.y + lax.rem(o, 4), 4)
            total = jnp.zeros((REST, BLK), BF16)
            slot = jnp.zeros((1, BLK), I32)
            for h in range(2):
                meta = arr_mb[n, h]
                base = lax.rem(meta[4:5, :], 16) + 1
                for a in range(4):
                    p = meta[a : a + 1, :]
                    hit = lax.div(p, 8) == r
                    mask = jnp.where(hit, F32(1.0), F32(0.0)).astype(BF16)
                    total = total + arr_b[n, h, a * REST : (a + 1) * REST, :] * mask
                    slot = jnp.where(hit, base + lax.rem(p, 8) * 16, slot)
            pk_b[o, n] = total
            pk_mb[o] = pk_mb[o] + jnp.where(lanes == n, slot, 0)
            return inside

        return lax.fori_loop(0, 16, each, carry)

    own_out = []

    def keep(src, dst, n):
        copy = pltpu.make_async_copy(src, dst, local.at[n])
        copy.start()
        own_out.append(copy)

    def second_a(g):
        part = pl.ds(4 * g, 4)
        for n in range(4 * g, 4 * g + 4):
            if n:
                wait_in(arr_ma.at[n], ma1r.at[n])
                wait_in(arr_a.at[n], a1r.at[n])
        lax.fori_loop(4 * g, 4 * g + 4, pack_a, 0)
        for o in range(1, 8):
            n = o * 4 + g
            go(
                remote(
                    pk_a.at[o, part], a2.at[o, part], a2s.at[n], a2r.at[n],
                    row, at.col_at(*COL_OFFS[o]),
                )
            )
        keep(pk_a.at[0, part], a2.at[0, part], 2 + g)

    def second_b(g):
        part = pl.ds(4 * g, 4)
        for n in range(4 * g, 4 * g + 4):
            if n:
                wait_in(arr_mb.at[n], mb1r.at[n])
                wait_in(arr_b.at[n], b1r.at[n])
        lax.fori_loop(4 * g, 4 * g + 4, pack_b, 0)
        for o in range(1, 16):
            n = o * 2 + g
            go(
                remote(
                    pk_b.at[o, part], b2.at[o, part], b2s.at[n], b2r.at[n],
                    at.row_at(*ROW_OFFS[o]), col,
                )
            )
        keep(pk_b.at[0, part], b2.at[0, part], 6 + g)

    second_a(0)
    second_b(0)
    second_a(1)
    second_b(1)
    for o in range(1, 16):
        go(remote(pk_mb.at[o], mb2.at[o], mb2s.at[o], mb2r.at[o], at.row_at(*ROW_OFFS[o]), col))
    for t in range(3):

        @pl.when(jnp.logical_and(inner, place == t + 1))
        def _():
            wait_in(rm.at[third(t)], rmr.at[t])
            for u in range(3):
                if u != t:
                    onward(t, u).start()
            across(t).start()

    second_a(2)
    second_a(3)
    for o in range(1, 8):
        go(remote(pk_ma.at[o], ma2.at[o], ma2s.at[o], ma2r.at[o], row, at.col_at(*COL_OFFS[o])))
    keep(pk_ma.at[0], ma2.at[0], 8)
    keep(pk_mb.at[0], mb2.at[0], 9)
    for t in range(3):

        @pl.when(jnp.logical_and(inner, place != t + 1))
        def _():
            wait_in(rm.at[third(t)], rmr.at[t])
            across(t).start()

    for o in range(1, 8):
        for g in range(4):
            wait_in(a2.at[o, pl.ds(4 * g, 4)], a2r.at[o * 4 + g])
        wait_in(ma2.at[o], ma2r.at[o])
    for o in range(1, 16):
        for g in range(2):
            wait_in(b2.at[o, pl.ds(4 * g, 4)], b2r.at[o * 2 + g])
        wait_in(mb2.at[o], mb2r.at[o])
    for copy in own_out:
        copy.wait()
    for t in range(3):

        @pl.when(root)
        def _():
            out_third(t).wait_send()

        @pl.when(on_lane)
        def _():
            across(t).wait_send()

        @pl.when(jnp.logical_not(on_lane))
        def _():
            across(t).wait_recv()

        @pl.when(jnp.logical_and(inner, place == t + 1))
        def _():
            for u in range(3):
                if u != t:
                    onward(t, u).wait_send()

    for copy in sends:
        copy.wait_send()


def exchange(block_map, inv_interior, coupling, boundary_stiff, mass_interior, mass_boundary, modes_t):
    subs, inside, edge = coupling.shape
    return pl.pallas_call(
        exchange_kernel,
        in_specs=[pl.BlockSpec(memory_space=pltpu.SMEM), ANY, ANY, ANY, VMEM, VMEM, ANY],
        out_specs=[ANY] * 6,
        out_shape=[
            jax.ShapeDtypeStruct((8, 16, BLK + LIFT, BLK), BF16),
            jax.ShapeDtypeStruct((16, 8, REST, BLK), BF16),
            jax.ShapeDtypeStruct((8, 8, BLK), I32),
            jax.ShapeDtypeStruct((16, 8, BLK), I32),
            jax.ShapeDtypeStruct((2, 16, 64, 1024), BF16),
            jax.ShapeDtypeStruct((16, 64, 1024), BF16),
        ],
        scratch_shapes=[
            pltpu.VMEM((subs, inside, inside), BF16),
            pltpu.VMEM((subs, inside, edge), BF16),
            pltpu.VMEM((subs, edge, edge), BF16),
            pltpu.VMEM((16, BLK + LIFT, edge), BF16),
            pltpu.VMEM((16, 4 * REST, BLK), BF16),
            pltpu.VMEM((16, BLK + LIFT, edge), BF16),
            pltpu.VMEM((8, 2, 4 * REST, BLK), BF16),
            pltpu.VMEM((16, 8, BLK), I32),
            pltpu.VMEM((8, 2, 8, BLK), I32),
            pltpu.VMEM((16, BLK + LIFT, edge), BF16),
            pltpu.VMEM((8, 2, 4 * REST, BLK), BF16),
            pltpu.VMEM((16, 8, BLK), I32),
            pltpu.VMEM((8, 2, 8, BLK), I32),
            pltpu.VMEM((8, 16, BLK + LIFT, BLK), BF16),
            pltpu.VMEM((16, 8, REST, BLK), BF16),
            pltpu.VMEM((8, 8, BLK), I32),
            pltpu.VMEM((16, 8, BLK), I32),
            DMA((3, 4)),
            DMA((16,)), DMA((16,)), DMA((8,)), DMA((8,)),
            DMA((16,)), DMA((16,)), DMA((8,)), DMA((8,)),
            DMA((32,)), DMA((32,)), DMA((32,)), DMA((32,)),
            DMA((8,)), DMA((8,)), DMA((16,)), DMA((16,)),
            DMA((6,)), DMA((6,)), DMA((24,)), DMA((24,)),
            DMA((3,)), DMA((3,)), DMA((3,)), DMA((3,)),
            DMA((10,)),
        ],
        compiler_params=pltpu.CompilerParams(
            collective_id=0, has_side_effects=True, vmem_limit_bytes=60 * 1024 * 1024
        ),
        name="exchange",
    )(block_map, inv_interior, coupling, boundary_stiff, mass_interior, mass_boundary, modes_t)


def assemble_kernel(
    a2, b2, ma2, mb2,
    stiff_out, mass_out, diag_out,
    va, vb, sa, sb, acc, tile, mass_tile, sems,
):
    at = Place()
    half = lax.rem(at.row, 2)
    holder = at.col == lax.div(at.row, 2)
    copies = [
        pltpu.make_async_copy(ma2, sa, sems.at[0]),
        pltpu.make_async_copy(a2, va, sems.at[1]),
        pltpu.make_async_copy(mb2, sb, sems.at[2]),
        pltpu.make_async_copy(b2, vb, sems.at[3]),
    ]
    for copy in copies:
        copy.start()

    def clear(n, carry):
        acc[n] = jnp.zeros((BLK, BLK), F32)
        return carry

    def gather_a(n, carry):
        for u in range(4):
            o, k = lax.div(n, 4), lax.rem(n, 4) * 4 + u
            slot = sa[o, 0, k]
            acc[slot] = acc[slot] + va[o, k, 0:BLK, :].astype(F32)
            lifted = acc[slot + 129, 0:LIFT, :] + va[o, k, BLK : BLK + LIFT, :].astype(F32)
            acc[slot + 129, 0:LIFT, :] = lifted
        return carry

    def gather_b(n, carry):
        for u in range(4):
            o, k = lax.div(n, 2), lax.rem(n, 2) * 4 + u
            slot = sb[o, 0, k] + 129
            acc[slot, LIFT:BLK, :] = acc[slot, LIFT:BLK, :] + vb[o, k].astype(F32)
        return carry

    def round_to(base, out):
        def one(p, carry):
            rows = pl.ds(pl.multiple_of(p * BLK, BLK), BLK)
            for q in range(16):
                out[rows, q * BLK : (q + 1) * BLK] = acc[base + p * 16 + q + 1].astype(BF16)
            return carry

        lax.fori_loop(0, 8, one, 0)

    lax.fori_loop(0, 258, clear, 0)
    copies[0].wait()
    copies[1].wait()
    lax.fori_loop(0, 32, gather_a, 0)
    round_to(0, tile)
    out_stiff = pltpu.make_async_copy(tile, stiff_out, sems.at[4])
    out_stiff.start()
    copies[2].wait()
    copies[3].wait()
    lax.fori_loop(0, 32, gather_b, 0)
    round_to(129, mass_tile)
    row_ids = lax.broadcasted_iota(I32, (BLK, BLK), 0)
    col_ids = lax.broadcasted_iota(I32, (BLK, BLK), 1)
    same = row_ids == col_ids

    @pl.when(holder)
    def _():
        for p in range(8):
            block = acc[130 + p * 17 + half * 8]
            line = jnp.sum(jnp.where(same, block, F32(0.0)), axis=0, keepdims=True)
            diag_out[p] = jnp.broadcast_to(line, (8, BLK))
            rest = jnp.where(same, F32(0.0), block).astype(BF16)
            start = pl.multiple_of(half * 1024 + p * BLK, BLK)
            mass_tile[p * BLK : (p + 1) * BLK, pl.ds(start, BLK)] = rest

    @pl.when(jnp.logical_not(holder))
    def _():
        diag_out[...] = jnp.zeros_like(diag_out)

    out_mass = pltpu.make_async_copy(mass_tile, mass_out, sems.at[5])
    out_mass.start()
    out_stiff.wait()
    out_mass.wait()


def assemble(a2, b2, ma2, mb2):
    return pl.pallas_call(
        assemble_kernel,
        in_specs=[ANY] * 4,
        out_specs=[ANY, ANY, VMEM],
        out_shape=[
            jax.ShapeDtypeStruct((1024, 2048), BF16),
            jax.ShapeDtypeStruct((1024, 2048), BF16),
            jax.ShapeDtypeStruct((8, 8, BLK), F32),
        ],
        scratch_shapes=[
            pltpu.VMEM((8, 16, BLK + LIFT, BLK), BF16),
            pltpu.VMEM((16, 8, REST, BLK), BF16),
            pltpu.SMEM((8, 8, BLK), I32),
            pltpu.SMEM((16, 8, BLK), I32),
            pltpu.VMEM((258, BLK, BLK), F32),
            pltpu.VMEM((1024, 2048), BF16),
            pltpu.VMEM((1024, 2048), BF16),
            DMA((6,)),
        ],
        compiler_params=pltpu.CompilerParams(vmem_limit_bytes=60 * 1024 * 1024),
        name="assemble",
    )(a2, b2, ma2, mb2)


GROUPS = ("zyx", "yxz", "xzy", "zyx")
WIDTH = 256


def reduce_kernel(
    stiff, mass, diag, cm, rm,
    stiff_out, mass_out, diag_out,
    tiles, vcm, vrm, *rest,
):
    bufs = [rest[7 * j : 7 * j + 7] for j in range(4)]
    send_last, arr_last = rest[28:30]
    ns, nr, s1, r1, s2, r2, s3, r3, ls, lr, ds, dr, local = rest[30:]
    at = Place()
    row, col = at.row, at.col
    half = lax.rem(row, 2)
    holder = col == lax.div(row, 2)
    mine = {"z": at.z, "y": at.y, "x": at.x}

    def remote(src, dst, ssem, rsem, r, c):
        return pltpu.make_async_remote_copy(
            src_ref=src, dst_ref=dst, send_sem=ssem, recv_sem=rsem,
            device_id=(r, c), device_id_type=MESH,
        )

    def away(axis, d):
        r = at.row_at(d if axis == "z" else 0, d if axis == "y" else 0)
        c = at.col_at(d if axis == "x" else 0, 0)
        return r, c, lax.rem(mine[axis] + d, 4)

    barrier = pltpu.get_barrier_semaphore()
    for d in range(1, 4):
        for axis in "zy":
            r, c, _ = away(axis, d)
            pl.semaphore_signal(barrier, inc=1, device_id=(r, c), device_id_type=MESH)
    for dx, dk in COL_OFFS[1:]:
        pl.semaphore_signal(barrier, inc=1, device_id=(row, at.col_at(dx, dk)), device_id_type=MESH)
    sibling = at.col_at(0, 1)
    depth = cm.shape[2]
    loads = [
        pltpu.make_async_copy(cm.at[h], vcm.at[:, pl.ds(h * depth, depth)], local.at[h])
        for h in range(2)
    ] + [
        pltpu.make_async_copy(stiff, tiles.at[0], local.at[2]),
        pltpu.make_async_copy(mass, tiles.at[1], local.at[3]),
    ]
    for copy in loads:
        copy.start()

    @pl.when(holder)
    def _():
        pltpu.make_async_copy(cm.at[half], vrm, local.at[4]).start()

    @pl.when(jnp.logical_not(holder))
    def _():
        pltpu.make_async_copy(rm, vrm, local.at[4]).start()

    for copy in loads:
        copy.wait()
    pltpu.make_async_copy(rm, vrm, local.at[4]).wait()

    @pl.when(holder)
    def _():
        row_ids = lax.broadcasted_iota(I32, (BLK, BLK), 0)
        col_ids = lax.broadcasted_iota(I32, (BLK, BLK), 1)
        for p in range(8):
            spot = (
                1,
                slice(p * BLK, (p + 1) * BLK),
                pl.ds(pl.multiple_of(half * 1024 + p * BLK, BLK), BLK),
            )
            block = tiles[spot].astype(F32)
            tiles[spot] = jnp.where(row_ids == col_ids, diag[p, 0:1, :], block).astype(BF16)

    pl.semaphore_wait(barrier, 13)

    def diag_copy(o):
        c = at.col_at(*COL_OFFS[o])
        return remote(diag.at[c], diag_out, ds.at[o], dr.at[0], row, c)

    @pl.when(holder)
    def _():
        for o in range(1, 8):
            diag_copy(o).start()
        own = pltpu.make_async_copy(diag.at[col], diag_out, local.at[5])
        own.start()
        own.wait()

    def product(which, pair):
        modes = vcm[pair * 2 * WIDTH : (pair + 1) * 2 * WIDTH, :]
        image = lax.dot_general(
            tiles[which], modes, (((1,), (1,)), ((), ())), preferred_element_type=F32
        )
        return jnp.dot(vrm[...], image.astype(BF16), preferred_element_type=F32)

    near = []
    for pair in range(2):
        theirs = product(1 - at.k, pair).astype(BF16)
        for side in range(2):
            j = pair * 2 + side
            out_near, in_near = bufs[j][:2]
            out_near[...] = theirs[:, side * WIDTH : (side + 1) * WIDTH]
            copy = remote(out_near, in_near, ns.at[j], nr.at[j], row, sibling)
            copy.start()
            near.append(copy)
    sends = []

    def leg(j, level, src, dst, ssem, rsem):
        axis = GROUPS[j][level]
        dims = sorted(GROUPS[j][level:], key="zyx".index)
        spot = dims.index(axis)
        arriving = []
        for d in range(1, 4):
            r, c, place = away(axis, d)
            part = src.at[(slice(None),) * spot + (place,)]
            copy = remote(part, dst.at[d], ssem.at[j * 4 + d], rsem.at[j * 4 + d], r, c)
            copy.start()
            sends.append(copy)
            arriving.append(copy)
        return arriving, (slice(None),) * spot + (mine[axis],)

    def summed(src, own, dst, arriving):
        for copy in arriving:
            copy.wait_recv()
        total = src[own].astype(F32)
        for d in range(1, 4):
            total = total + dst[d].astype(F32)
        return total

    first_legs = []
    for pair in range(2):
        ours = product(at.k, pair)
        for side in range(2):
            j = pair * 2 + side
            _, in_near, near_sum, arr1, _, _, _ = bufs[j]
            near[j].wait_recv()
            total = ours[:, side * WIDTH : (side + 1) * WIDTH] + in_near[...].astype(F32)
            near_sum[...] = total.astype(BF16).reshape(4, 4, 4, 16, WIDTH)
            first_legs.append(leg(j, 0, near_sum, arr1, s1, r1))
    second_legs = []
    for j in range(4):
        _, _, near_sum, arr1, sum1, arr2, _ = bufs[j]
        arriving, own = first_legs[j]
        sum1[...] = summed(near_sum, own, arr1, arriving).astype(BF16)
        second_legs.append(leg(j, 1, sum1, arr2, s2, r2))
    third_legs = []
    for j in range(4):
        sum1, arr2, last = bufs[j][4:]
        arriving, own = second_legs[j]
        last[0] = summed(sum1, own, arr2, arriving).astype(BF16)
        third_legs.append(leg(j, 2, last.at[0], last.at[1], s3, r3))
    for j in range(4):
        last = bufs[j][6]
        arriving, own = third_legs[j]
        total = summed(last.at[0], own, last.at[1], arriving)
        cols = slice(j * WIDTH, (j + 1) * WIDTH)
        send_last[0, :, cols] = total[0:8, :]
        send_last[1, :, cols] = total[8:16, :]
    final = remote(send_last.at[1 - at.k], arr_last, ls.at[0], lr.at[0], row, sibling)
    final.start()
    final.wait_recv()
    kept = send_last[at.k]
    got = arr_last[...]
    lower = at.k == 0
    stiff_out[...] = jnp.where(lower, kept, got)
    mass_out[...] = jnp.where(lower, got, kept)

    @pl.when(jnp.logical_not(holder))
    def _():
        diag_copy(0).wait_recv()

    @pl.when(holder)
    def _():
        for o in range(1, 8):
            diag_copy(o).wait_send()

    for copy in near + sends + [final]:
        copy.wait_send()


def reduce_parts(stiff, mass, diag, cm, rm):
    scratch = [
        pltpu.VMEM((2, 1024, 2048), BF16),
        pltpu.VMEM((1024, 2048), BF16),
        pltpu.VMEM((1024, 1024), BF16),
    ]
    for _ in GROUPS:
        scratch += [
            pltpu.VMEM((1024, WIDTH), BF16),
            pltpu.VMEM((1024, WIDTH), BF16),
            pltpu.VMEM((4, 4, 4, 16, WIDTH), BF16),
            pltpu.VMEM((4, 4, 4, 16, WIDTH), BF16),
            pltpu.VMEM((4, 4, 16, WIDTH), BF16),
            pltpu.VMEM((4, 4, 16, WIDTH), BF16),
            pltpu.VMEM((2, 4, 16, WIDTH), BF16),
        ]
    return pl.pallas_call(
        reduce_kernel,
        in_specs=[ANY, ANY, VMEM, ANY, ANY],
        out_specs=[VMEM, VMEM, VMEM],
        out_shape=[
            jax.ShapeDtypeStruct((8, 1024), F32),
            jax.ShapeDtypeStruct((8, 1024), F32),
            jax.ShapeDtypeStruct((8, BLK), F32),
        ],
        scratch_shapes=scratch
        + [
            pltpu.VMEM((2, 8, 1024), F32),
            pltpu.VMEM((8, 1024), F32),
            DMA((4,)), DMA((4,)),
            DMA((16,)), DMA((16,)), DMA((16,)), DMA((16,)), DMA((16,)), DMA((16,)),
            DMA((1,)), DMA((1,)), DMA((8,)), DMA((1,)), DMA((6,)),
        ],
        compiler_params=pltpu.CompilerParams(
            collective_id=1, has_side_effects=True, vmem_limit_bytes=60 * 1024 * 1024
        ),
        name="reduce",
    )(stiff, mass, diag, cm, rm)


def body(inv_interior, coupling, boundary_stiff, mass_interior, mass_boundary, block_map, modes):
    a2, b2, ma2, mb2, cm, rm = exchange(
        block_map, inv_interior, coupling, boundary_stiff, mass_interior, mass_boundary, modes.T
    )
    stiff_tile, mass_tile, diag = assemble(a2, b2, ma2, mb2)
    stiff, mass, diagonal = reduce_parts(
        stiff_tile, mass_tile, diag, cm.reshape(2, 1024, 1024), rm.reshape(1024, 1024)
    )
    return stiff_tile, mass_tile, stiff, mass, diagonal[0]


def solution(mesh):
    both = ("row", "col")
    return jax.shard_map(
        body,
        mesh=mesh,
        in_specs=(
            P(both, None, None),
            P(both, None, None),
            P(both, None, None),
            P(both, None),
            P(both, None),
            P(both, None),
            P("col", "row"),
        ),
        out_specs=(
            P("row", "col"),
            P("row", "col"),
            P(both, None),
            P(both, None),
            P(both),
        ),
        check_vma=False,
    )
```

```python
import functools

import jax
import jax.numpy as jnp
from jax import lax
from jax.experimental import pallas as pl
from jax.experimental.pallas import tpu as pltpu
from jax.sharding import PartitionSpec as P

MESH = pl.DeviceIdType.MESH
BLK = 128
LIFT = 16
REST = BLK - LIFT
F32 = jnp.float32
BF16 = jnp.bfloat16
I32 = jnp.int32
ANY = pl.BlockSpec(memory_space=pl.ANY)
VMEM = pl.BlockSpec(memory_space=pltpu.VMEM)
DMA = pltpu.SemaphoreType.DMA
ROW_OFFS = [(dz, dy) for dz in range(4) for dy in range(4)]
COL_OFFS = [(dx, dk) for dx in range(4) for dk in range(2)]


class Place:
    def __init__(self):
        self.row = lax.axis_index("row")
        self.col = lax.axis_index("col")
        self.z, self.y = lax.div(self.row, 4), lax.rem(self.row, 4)
        self.x, self.k = lax.div(self.col, 2), lax.rem(self.col, 2)

    def row_at(self, dz, dy):
        return lax.rem(self.z + dz, 4) * 4 + lax.rem(self.y + dy, 4)

    def col_at(self, dx, dk):
        return lax.rem(self.x + dx, 4) * 2 + lax.rem(self.k + dk, 2)


THIRDS = ((0, 6), (6, 4), (10, 6))


def exchange_kernel(
    map_ref, inv, couple, stiff, mi_ref, mb_ref, modes_t,
    a2, b2, ma2, mb2, cm, rm,
    v_inv, v_couple, v_stiff, nat_a, nat_b, st_a, st_b, st_ma, st_mb,
    arr_a, arr_b, arr_ma, arr_mb, pk_a, pk_b, pk_ma, pk_mb,
    lds, a1s, a1r, b1s, b1r, ma1s, ma1r, mb1s, mb1r,
    a2s, a2r, b2s, b2r, ma2s, ma2r, mb2s, mb2r,
    m1s, m1r, m2s, m2r, rms, rmr, sbs, sbr, local,
):
    at = Place()
    row, col = at.row, at.col

    def remote(src, dst, ssem, rsem, r, c):
        return pltpu.make_async_remote_copy(
            src_ref=src, dst_ref=dst, send_sem=ssem, recv_sem=rsem,
            device_id=(r, c), device_id_type=MESH,
        )

    barrier = pltpu.get_barrier_semaphore()
    for dz, dy in ROW_OFFS[1:]:
        pl.semaphore_signal(barrier, inc=1, device_id=(at.row_at(dz, dy), col), device_id_type=MESH)
    for dx, dk in COL_OFFS[1:]:
        pl.semaphore_signal(barrier, inc=1, device_id=(row, at.col_at(dx, dk)), device_id_type=MESH)

    def loads(s):
        return [
            pltpu.make_async_copy(inv.at[s], v_inv.at[s], lds.at[0, s]),
            pltpu.make_async_copy(couple.at[s], v_couple.at[s], lds.at[1, s]),
            pltpu.make_async_copy(stiff.at[s], v_stiff.at[s], lds.at[2, s]),
        ]

    for s in range(4):
        for copy in loads(s):
            copy.start()
    own_modes = [
        pltpu.make_async_copy(modes_t.at[:, pl.ds(h * 1024, 1024)], cm.at[h, row], local.at[h])
        for h in range(2)
    ]
    for copy in own_modes:
        copy.start()

    sends = []

    def go(copy):
        copy.start()
        sends.append(copy)

    def wait_in(dst, rsem):
        remote(dst, dst, rsem, rsem, row, col).wait_recv()

    def condense(s, carry):
        for copy in loads(s):
            copy.wait()
        pair = v_couple[s]
        static = (-jnp.dot(v_inv[s], pair, preferred_element_type=F32)).astype(BF16)
        stiffness = v_stiff[s].astype(F32) + lax.dot_general(
            pair, static, (((0,), (0,)), ((), ())), preferred_element_type=F32
        )
        stiffness = stiffness.astype(BF16)
        for a in range(4):
            nat_a[s * 4 + a, 0:BLK, :] = stiffness[a * BLK : (a + 1) * BLK, :]
        static_t = static.T
        weighted_t = (static_t.astype(F32) * mi_ref[pl.ds(s, 1), :]).astype(BF16)
        mass = lax.dot_general(
            static_t, weighted_t, (((1,), (1,)), ((), ())), preferred_element_type=F32
        )
        width = mass.shape[0]
        row_ids = lax.broadcasted_iota(I32, (width, width), 0)
        col_ids = lax.broadcasted_iota(I32, (width, width), 1)
        mass = mass + jnp.where(row_ids == col_ids, mb_ref[pl.ds(s, 1), :], F32(0.0))
        mass = mass.astype(BF16)
        for a in range(4):
            lifted = a * BLK + LIFT
            nat_a[s * 4 + a, BLK : BLK + LIFT, :] = mass[a * BLK : lifted, :]
            for b in range(4):
                nat_b[s * 4 + b, a * REST : (a + 1) * REST, :] = mass[
                    lifted : (a + 1) * BLK, b * BLK : (b + 1) * BLK
                ]
        return carry

    pl.semaphore_wait(barrier, 22)
    for d in (1, 3, 2):
        for h in range(2):
            r = at.row_at(d, 0) if h == 0 else at.row_at(0, d)
            n = h * 3 + d - 1
            go(
                remote(
                    modes_t.at[:, pl.ds(h * 1024, 1024)], cm.at[h, row],
                    m1s.at[n], m1r.at[n], r, col,
                )
            )
    lax.fori_loop(0, 2, condense, 0)
    for copy in own_modes:
        copy.wait()
    for d in (0, 1, 3, 2):
        for h in range(2):
            if d:
                back = at.row_at(4 - d, 0) if h == 0 else at.row_at(0, 4 - d)
                wait_in(cm.at[h, back], m1r.at[h * 3 + d - 1])
            else:
                back = row
            for e in (1, 3, 2):
                r = at.row_at(0, e) if h == 0 else at.row_at(e, 0)
                n = h * 12 + d * 3 + e - 1
                go(remote(cm.at[h, back], cm.at[h, back], m2s.at[n], m2r.at[n], r, col))
    lax.fori_loop(2, 4, condense, 0)

    lines = lax.broadcasted_iota(I32, (8, BLK), 0)

    def find(tile_row):
        found = jnp.int32(0)
        for n in range(16):
            found = jnp.where(lax.div(map_ref[n // 4, n % 4], 8) == tile_row, n, found)
        sub = lax.div(found, 4)
        table = jnp.full((8, BLK), map_ref[sub, lax.rem(found, 4)], I32)
        for a in range(4):
            table = jnp.where(lines == a, map_ref[sub, a], table)
        return found, table

    def stage_a(o, carry):
        r = lax.rem(at.z + lax.div(o, 4), 4) * 4 + lax.rem(at.y + lax.rem(o, 4), 4)
        found, table = find(r)
        st_a[o] = nat_a[found]
        st_ma[o] = table
        return carry

    def stage_b(o, carry):
        n, h = lax.div(o, 2), lax.rem(o, 2)
        c = lax.rem(at.x + lax.div(n, 2), 4) * 2 + lax.rem(at.k + lax.rem(n, 2), 2)
        found, table = find(2 * c + h)
        st_b[n, h] = nat_b[found]
        st_mb[n, h] = table
        return carry

    lax.fori_loop(0, 16, stage_b, 0)
    for n in range(1, 8):
        c = at.col_at(*COL_OFFS[n])
        go(remote(st_mb.at[n], arr_mb.at[n], mb1s.at[n], mb1r.at[n], row, c))
        go(remote(st_b.at[n], arr_b.at[n], b1s.at[n], b1r.at[n], row, c))
    lax.fori_loop(0, 16, stage_a, 0)
    for n in range(1, 16):
        r = at.row_at(*ROW_OFFS[n])
        go(remote(st_ma.at[n], arr_ma.at[n], ma1s.at[n], ma1r.at[n], r, col))
        go(remote(st_a.at[n], arr_a.at[n], a1s.at[n], a1r.at[n], r, col))
    arr_a[0] = st_a[0]
    arr_ma[0] = st_ma[0]
    arr_b[0] = st_b[0]
    arr_mb[0] = st_mb[0]
    pk_ma[...] = jnp.zeros_like(pk_ma)
    pk_mb[...] = jnp.zeros_like(pk_mb)
    lanes = lax.broadcasted_iota(I32, (8, BLK), 1)

    for d in (0, 1, 3, 2):
        for h in range(2):
            for e in (1, 3, 2):
                back = at.row_at(4 - d, 4 - e) if h == 0 else at.row_at(4 - e, 4 - d)
                wait_in(cm.at[h, back], m2r.at[h * 12 + d * 3 + e - 1])
    half = lax.rem(row, 2)
    on_lane = at.k == lax.div(at.y, 2)
    place = lax.rem(at.x + 4 - at.z, 4)
    root = jnp.logical_and(on_lane, place == 0)
    inner = jnp.logical_and(on_lane, place > 0)
    sibling = at.col_at(0, 1)

    def third(t):
        return pl.ds(THIRDS[t][0], THIRDS[t][1])

    def out_third(t):
        return remote(
            cm.at[half, third(t)], rm.at[third(t)], rms.at[t], rmr.at[t], row, at.col_at(t + 1, 0)
        )

    def root_across(t):
        return remote(
            cm.at[half, third(t)], rm.at[third(t)], sbs.at[t], sbr.at[t], row, sibling
        )

    def across(t):
        return remote(rm.at[third(t)], rm.at[third(t)], sbs.at[t], sbr.at[t], row, sibling)

    def onward(t, u):
        return remote(
            rm.at[third(t)], rm.at[third(t)], rms.at[u], rmr.at[t], row, at.col_at(u + 4 - t, 0)
        )

    @pl.when(root)
    def _():
        for t in range(3):
            out_third(t).start()
            root_across(t).start()

    def pack_a(n, carry):
        meta = arr_ma[n]
        base = lax.rem(meta[4:5, :], 8) * 16 + 1
        for o in range(8):
            c = at.col_at(*COL_OFFS[o])
            total = jnp.zeros((BLK + LIFT, BLK), BF16)
            slot = jnp.zeros((1, BLK), I32)
            for b in range(4):
                q = meta[b : b + 1, :]
                hit = lax.div(q, 16) == c
                mask = jnp.where(hit, F32(1.0), F32(0.0)).astype(BF16)
                total = total + arr_a[n, :, b * BLK : (b + 1) * BLK] * mask
                slot = jnp.where(hit, base + lax.rem(q, 16), slot)
            pk_a[o, n] = total
            pk_ma[o] = pk_ma[o] + jnp.where(lanes == n, slot, 0)
        return carry

    def pack_b(n, carry):
        def each(o, inside):
            r = lax.rem(at.z + lax.div(o, 4), 4) * 4 + lax.rem(at.y + lax.rem(o, 4), 4)
            total = jnp.zeros((REST, BLK), BF16)
            slot = jnp.zeros((1, BLK), I32)
            for h in range(2):
                meta = arr_mb[n, h]
                base = lax.rem(meta[4:5, :], 16) + 1
                for a in range(4):
                    p = meta[a : a + 1, :]
                    hit = lax.div(p, 8) == r
                    mask = jnp.where(hit, F32(1.0), F32(0.0)).astype(BF16)
                    total = total + arr_b[n, h, a * REST : (a + 1) * REST, :] * mask
                    slot = jnp.where(hit, base + lax.rem(p, 8) * 16, slot)
            pk_b[o, n] = total
            pk_mb[o] = pk_mb[o] + jnp.where(lanes == n, slot, 0)
            return inside

        return lax.fori_loop(0, 16, each, carry)

    own_out = []

    def keep(src, dst, n):
        copy = pltpu.make_async_copy(src, dst, local.at[n])
        copy.start()
        own_out.append(copy)

    def second_a(g):
        part = pl.ds(4 * g, 4)
        for n in range(4 * g, 4 * g + 4):
            if n:
                wait_in(arr_ma.at[n], ma1r.at[n])
                wait_in(arr_a.at[n], a1r.at[n])
        lax.fori_loop(4 * g, 4 * g + 4, pack_a, 0)
        for o in range(1, 8):
            n = o * 4 + g
            go(
                remote(
                    pk_a.at[o, part], a2.at[o, part], a2s.at[n], a2r.at[n],
                    row, at.col_at(*COL_OFFS[o]),
                )
            )
        keep(pk_a.at[0, part], a2.at[0, part], 2 + g)

    def second_b(g):
        part = pl.ds(4 * g, 4)
        for n in range(4 * g, 4 * g + 4):
            if n:
                wait_in(arr_mb.at[n], mb1r.at[n])
                wait_in(arr_b.at[n], b1r.at[n])
        lax.fori_loop(4 * g, 4 * g + 4, pack_b, 0)
        for o in range(1, 16):
            n = o * 2 + g
            go(
                remote(
                    pk_b.at[o, part], b2.at[o, part], b2s.at[n], b2r.at[n],
                    at.row_at(*ROW_OFFS[o]), col,
                )
            )
        keep(pk_b.at[0, part], b2.at[0, part], 6 + g)

    second_a(0)
    second_b(0)
    second_a(1)
    second_b(1)
    for o in range(1, 16):
        go(remote(pk_mb.at[o], mb2.at[o], mb2s.at[o], mb2r.at[o], at.row_at(*ROW_OFFS[o]), col))
    for t in range(3):

        @pl.when(jnp.logical_and(inner, place == t + 1))
        def _():
            wait_in(rm.at[third(t)], rmr.at[t])
            for u in range(3):
                if u != t:
                    onward(t, u).start()
            across(t).start()

    second_a(2)
    second_a(3)
    for o in range(1, 8):
        go(remote(pk_ma.at[o], ma2.at[o], ma2s.at[o], ma2r.at[o], row, at.col_at(*COL_OFFS[o])))
    keep(pk_ma.at[0], ma2.at[0], 8)
    keep(pk_mb.at[0], mb2.at[0], 9)
    for t in range(3):

        @pl.when(jnp.logical_and(inner, place != t + 1))
        def _():
            wait_in(rm.at[third(t)], rmr.at[t])
            across(t).start()

    for o in range(1, 8):
        for g in range(4):
            wait_in(a2.at[o, pl.ds(4 * g, 4)], a2r.at[o * 4 + g])
        wait_in(ma2.at[o], ma2r.at[o])
    for o in range(1, 16):
        for g in range(2):
            wait_in(b2.at[o, pl.ds(4 * g, 4)], b2r.at[o * 2 + g])
        wait_in(mb2.at[o], mb2r.at[o])
    for copy in own_out:
        copy.wait()
    for t in range(3):

        @pl.when(root)
        def _():
            out_third(t).wait_send()

        @pl.when(on_lane)
        def _():
            across(t).wait_send()

        @pl.when(jnp.logical_not(on_lane))
        def _():
            across(t).wait_recv()

        @pl.when(jnp.logical_and(inner, place == t + 1))
        def _():
            for u in range(3):
                if u != t:
                    onward(t, u).wait_send()

    for copy in sends:
        copy.wait_send()


def exchange(block_map, inv_interior, coupling, boundary_stiff, mass_interior, mass_boundary, modes_t):
    subs, inside, edge = coupling.shape
    return pl.pallas_call(
        exchange_kernel,
        in_specs=[pl.BlockSpec(memory_space=pltpu.SMEM), ANY, ANY, ANY, VMEM, VMEM, ANY],
        out_specs=[ANY] * 6,
        out_shape=[
            jax.ShapeDtypeStruct((8, 16, BLK + LIFT, BLK), BF16),
            jax.ShapeDtypeStruct((16, 8, REST, BLK), BF16),
            jax.ShapeDtypeStruct((8, 8, BLK), I32),
            jax.ShapeDtypeStruct((16, 8, BLK), I32),
            jax.ShapeDtypeStruct((2, 16, 64, 1024), BF16),
            jax.ShapeDtypeStruct((16, 64, 1024), BF16),
        ],
        scratch_shapes=[
            pltpu.VMEM((subs, inside, inside), BF16),
            pltpu.VMEM((subs, inside, edge), BF16),
            pltpu.VMEM((subs, edge, edge), BF16),
            pltpu.VMEM((16, BLK + LIFT, edge), BF16),
            pltpu.VMEM((16, 4 * REST, BLK), BF16),
            pltpu.VMEM((16, BLK + LIFT, edge), BF16),
            pltpu.VMEM((8, 2, 4 * REST, BLK), BF16),
            pltpu.VMEM((16, 8, BLK), I32),
            pltpu.VMEM((8, 2, 8, BLK), I32),
            pltpu.VMEM((16, BLK + LIFT, edge), BF16),
            pltpu.VMEM((8, 2, 4 * REST, BLK), BF16),
            pltpu.VMEM((16, 8, BLK), I32),
            pltpu.VMEM((8, 2, 8, BLK), I32),
            pltpu.VMEM((8, 16, BLK + LIFT, BLK), BF16),
            pltpu.VMEM((16, 8, REST, BLK), BF16),
            pltpu.VMEM((8, 8, BLK), I32),
            pltpu.VMEM((16, 8, BLK), I32),
            DMA((3, 4)),
            DMA((16,)), DMA((16,)), DMA((8,)), DMA((8,)),
            DMA((16,)), DMA((16,)), DMA((8,)), DMA((8,)),
            DMA((32,)), DMA((32,)), DMA((32,)), DMA((32,)),
            DMA((8,)), DMA((8,)), DMA((16,)), DMA((16,)),
            DMA((6,)), DMA((6,)), DMA((24,)), DMA((24,)),
            DMA((3,)), DMA((3,)), DMA((3,)), DMA((3,)),
            DMA((10,)),
        ],
        compiler_params=pltpu.CompilerParams(
            collective_id=0, has_side_effects=True, vmem_limit_bytes=60 * 1024 * 1024
        ),
        name="exchange",
    )(block_map, inv_interior, coupling, boundary_stiff, mass_interior, mass_boundary, modes_t)


def assemble_kernel(
    a2, b2, ma2, mb2,
    stiff_out, mass_out, diag_out,
    va, vb, sa, sb, acc, tile, mass_tile, sems,
):
    at = Place()
    half = lax.rem(at.row, 2)
    holder = at.col == lax.div(at.row, 2)
    copies = [
        pltpu.make_async_copy(ma2, sa, sems.at[0]),
        pltpu.make_async_copy(a2, va, sems.at[1]),
        pltpu.make_async_copy(mb2, sb, sems.at[2]),
        pltpu.make_async_copy(b2, vb, sems.at[3]),
    ]
    for copy in copies:
        copy.start()

    def clear(n, carry):
        acc[n] = jnp.zeros((BLK, BLK), F32)
        return carry

    def gather_a(n, carry):
        for u in range(4):
            o, k = lax.div(n, 4), lax.rem(n, 4) * 4 + u
            slot = sa[o, 0, k]
            acc[slot] = acc[slot] + va[o, k, 0:BLK, :].astype(F32)
            lifted = acc[slot + 129, 0:LIFT, :] + va[o, k, BLK : BLK + LIFT, :].astype(F32)
            acc[slot + 129, 0:LIFT, :] = lifted
        return carry

    def gather_b(n, carry):
        for u in range(4):
            o, k = lax.div(n, 2), lax.rem(n, 2) * 4 + u
            slot = sb[o, 0, k] + 129
            acc[slot, LIFT:BLK, :] = acc[slot, LIFT:BLK, :] + vb[o, k].astype(F32)
        return carry

    def round_to(base, out):
        def one(p, carry):
            rows = pl.ds(pl.multiple_of(p * BLK, BLK), BLK)
            for q in range(16):
                out[rows, q * BLK : (q + 1) * BLK] = acc[base + p * 16 + q + 1].astype(BF16)
            return carry

        lax.fori_loop(0, 8, one, 0)

    lax.fori_loop(0, 258, clear, 0)
    copies[0].wait()
    copies[1].wait()
    lax.fori_loop(0, 32, gather_a, 0)
    round_to(0, tile)
    out_stiff = pltpu.make_async_copy(tile, stiff_out, sems.at[4])
    out_stiff.start()
    copies[2].wait()
    copies[3].wait()
    lax.fori_loop(0, 32, gather_b, 0)
    round_to(129, mass_tile)
    row_ids = lax.broadcasted_iota(I32, (BLK, BLK), 0)
    col_ids = lax.broadcasted_iota(I32, (BLK, BLK), 1)
    same = row_ids == col_ids

    @pl.when(holder)
    def _():
        for p in range(8):
            block = acc[130 + p * 17 + half * 8]
            line = jnp.sum(jnp.where(same, block, F32(0.0)), axis=0, keepdims=True)
            diag_out[p] = jnp.broadcast_to(line, (8, BLK))
            rest = jnp.where(same, F32(0.0), block).astype(BF16)
            start = pl.multiple_of(half * 1024 + p * BLK, BLK)
            mass_tile[p * BLK : (p + 1) * BLK, pl.ds(start, BLK)] = rest

    @pl.when(jnp.logical_not(holder))
    def _():
        diag_out[...] = jnp.zeros_like(diag_out)

    out_mass = pltpu.make_async_copy(mass_tile, mass_out, sems.at[5])
    out_mass.start()
    out_stiff.wait()
    out_mass.wait()


def assemble(a2, b2, ma2, mb2):
    return pl.pallas_call(
        assemble_kernel,
        in_specs=[ANY] * 4,
        out_specs=[ANY, ANY, VMEM],
        out_shape=[
            jax.ShapeDtypeStruct((1024, 2048), BF16),
            jax.ShapeDtypeStruct((1024, 2048), BF16),
            jax.ShapeDtypeStruct((8, 8, BLK), F32),
        ],
        scratch_shapes=[
            pltpu.VMEM((8, 16, BLK + LIFT, BLK), BF16),
            pltpu.VMEM((16, 8, REST, BLK), BF16),
            pltpu.SMEM((8, 8, BLK), I32),
            pltpu.SMEM((16, 8, BLK), I32),
            pltpu.VMEM((258, BLK, BLK), F32),
            pltpu.VMEM((1024, 2048), BF16),
            pltpu.VMEM((1024, 2048), BF16),
            DMA((6,)),
        ],
        compiler_params=pltpu.CompilerParams(vmem_limit_bytes=60 * 1024 * 1024),
        name="assemble",
    )(a2, b2, ma2, mb2)


GROUPS = ("zyx", "yxz", "xzy", "zyx")
WIDTH = 256


def reduce_kernel(
    stiff, mass, diag, cm, rm,
    stiff_out, mass_out, diag_out,
    tiles, vcm, vrm, *rest,
):
    bufs = [rest[7 * j : 7 * j + 7] for j in range(4)]
    send_last, arr_last = rest[28:30]
    ns, nr, s1, r1, s2, r2, s3, r3, ls, lr, ds, dr, local = rest[30:]
    at = Place()
    row, col = at.row, at.col
    half = lax.rem(row, 2)
    holder = col == lax.div(row, 2)
    mine = {"z": at.z, "y": at.y, "x": at.x}

    def remote(src, dst, ssem, rsem, r, c):
        return pltpu.make_async_remote_copy(
            src_ref=src, dst_ref=dst, send_sem=ssem, recv_sem=rsem,
            device_id=(r, c), device_id_type=MESH,
        )

    def away(axis, d):
        r = at.row_at(d if axis == "z" else 0, d if axis == "y" else 0)
        c = at.col_at(d if axis == "x" else 0, 0)
        return r, c, lax.rem(mine[axis] + d, 4)

    barrier = pltpu.get_barrier_semaphore()
    for d in range(1, 4):
        for axis in "zy":
            r, c, _ = away(axis, d)
            pl.semaphore_signal(barrier, inc=1, device_id=(r, c), device_id_type=MESH)
    for dx, dk in COL_OFFS[1:]:
        pl.semaphore_signal(barrier, inc=1, device_id=(row, at.col_at(dx, dk)), device_id_type=MESH)
    sibling = at.col_at(0, 1)
    depth = cm.shape[2]
    loads = [
        pltpu.make_async_copy(cm.at[h], vcm.at[:, pl.ds(h * depth, depth)], local.at[h])
        for h in range(2)
    ] + [
        pltpu.make_async_copy(stiff, tiles.at[0], local.at[2]),
        pltpu.make_async_copy(mass, tiles.at[1], local.at[3]),
    ]
    for copy in loads:
        copy.start()

    @pl.when(holder)
    def _():
        pltpu.make_async_copy(cm.at[half], vrm, local.at[4]).start()

    @pl.when(jnp.logical_not(holder))
    def _():
        pltpu.make_async_copy(rm, vrm, local.at[4]).start()

    for copy in loads:
        copy.wait()
    pltpu.make_async_copy(rm, vrm, local.at[4]).wait()

    @pl.when(holder)
    def _():
        row_ids = lax.broadcasted_iota(I32, (BLK, BLK), 0)
        col_ids = lax.broadcasted_iota(I32, (BLK, BLK), 1)
        for p in range(8):
            spot = (
                1,
                slice(p * BLK, (p + 1) * BLK),
                pl.ds(pl.multiple_of(half * 1024 + p * BLK, BLK), BLK),
            )
            block = tiles[spot].astype(F32)
            tiles[spot] = jnp.where(row_ids == col_ids, diag[p, 0:1, :], block).astype(BF16)

    pl.semaphore_wait(barrier, 13)

    def diag_copy(o):
        c = at.col_at(*COL_OFFS[o])
        return remote(diag.at[c], diag_out, ds.at[o], dr.at[0], row, c)

    @pl.when(holder)
    def _():
        for o in range(1, 8):
            diag_copy(o).start()
        own = pltpu.make_async_copy(diag.at[col], diag_out, local.at[5])
        own.start()
        own.wait()

    def product(which, pair):
        modes = vcm[pair * 2 * WIDTH : (pair + 1) * 2 * WIDTH, :]
        image = lax.dot_general(
            tiles[which], modes, (((1,), (1,)), ((), ())), preferred_element_type=F32
        )
        return jnp.dot(vrm[...], image.astype(BF16), preferred_element_type=F32)

    near = []
    for pair in range(2):
        theirs = product(1 - at.k, pair).astype(BF16)
        for side in range(2):
            j = pair * 2 + side
            out_near, in_near = bufs[j][:2]
            out_near[...] = theirs[:, side * WIDTH : (side + 1) * WIDTH]
            copy = remote(out_near, in_near, ns.at[j], nr.at[j], row, sibling)
            copy.start()
            near.append(copy)
    sends = []

    def leg(j, level, src, dst, ssem, rsem):
        axis = GROUPS[j][level]
        dims = sorted(GROUPS[j][level:], key="zyx".index)
        spot = dims.index(axis)
        arriving = []
        for d in range(1, 4):
            r, c, place = away(axis, d)
            part = src.at[(slice(None),) * spot + (place,)]
            copy = remote(part, dst.at[d], ssem.at[j * 4 + d], rsem.at[j * 4 + d], r, c)
            copy.start()
            sends.append(copy)
            arriving.append(copy)
        return arriving, (slice(None),) * spot + (mine[axis],)

    def summed(src, own, dst, arriving):
        for copy in arriving:
            copy.wait_recv()
        total = src[own].astype(F32)
        for d in range(1, 4):
            total = total + dst[d].astype(F32)
        return total

    first_legs = []
    for pair in range(2):
        ours = product(at.k, pair)
        for side in range(2):
            j = pair * 2 + side
            _, in_near, near_sum, arr1, _, _, _ = bufs[j]
            near[j].wait_recv()
            total = ours[:, side * WIDTH : (side + 1) * WIDTH] + in_near[...].astype(F32)
            near_sum[...] = total.astype(BF16).reshape(4, 4, 4, 16, WIDTH)
            first_legs.append(leg(j, 0, near_sum, arr1, s1, r1))
    second_legs = []
    for j in range(4):
        _, _, near_sum, arr1, sum1, arr2, _ = bufs[j]
        arriving, own = first_legs[j]
        sum1[...] = summed(near_sum, own, arr1, arriving).astype(BF16)
        second_legs.append(leg(j, 1, sum1, arr2, s2, r2))
    third_legs = []
    for j in range(4):
        sum1, arr2, last = bufs[j][4:]
        arriving, own = second_legs[j]
        last[0] = summed(sum1, own, arr2, arriving).astype(BF16)
        third_legs.append(leg(j, 2, last.at[0], last.at[1], s3, r3))
    for j in range(4):
        last = bufs[j][6]
        arriving, own = third_legs[j]
        total = summed(last.at[0], own, last.at[1], arriving)
        cols = slice(j * WIDTH, (j + 1) * WIDTH)
        send_last[0, :, cols] = total[0:8, :]
        send_last[1, :, cols] = total[8:16, :]
    final = remote(send_last.at[1 - at.k], arr_last, ls.at[0], lr.at[0], row, sibling)
    final.start()
    final.wait_recv()
    kept = send_last[at.k]
    got = arr_last[...]
    lower = at.k == 0
    stiff_out[...] = jnp.where(lower, kept, got)
    mass_out[...] = jnp.where(lower, got, kept)

    @pl.when(jnp.logical_not(holder))
    def _():
        diag_copy(0).wait_recv()

    @pl.when(holder)
    def _():
        for o in range(1, 8):
            diag_copy(o).wait_send()

    for copy in near + sends + [final]:
        copy.wait_send()


def reduce_parts(stiff, mass, diag, cm, rm):
    scratch = [
        pltpu.VMEM((2, 1024, 2048), BF16),
        pltpu.VMEM((1024, 2048), BF16),
        pltpu.VMEM((1024, 1024), BF16),
    ]
    for _ in GROUPS:
        scratch += [
            pltpu.VMEM((1024, WIDTH), BF16),
            pltpu.VMEM((1024, WIDTH), BF16),
            pltpu.VMEM((4, 4, 4, 16, WIDTH), BF16),
            pltpu.VMEM((4, 4, 4, 16, WIDTH), BF16),
            pltpu.VMEM((4, 4, 16, WIDTH), BF16),
            pltpu.VMEM((4, 4, 16, WIDTH), BF16),
            pltpu.VMEM((2, 4, 16, WIDTH), BF16),
        ]
    return pl.pallas_call(
        reduce_kernel,
        in_specs=[ANY, ANY, VMEM, ANY, ANY],
        out_specs=[VMEM, VMEM, VMEM],
        out_shape=[
            jax.ShapeDtypeStruct((8, 1024), F32),
            jax.ShapeDtypeStruct((8, 1024), F32),
            jax.ShapeDtypeStruct((8, BLK), F32),
        ],
        scratch_shapes=scratch
        + [
            pltpu.VMEM((2, 8, 1024), F32),
            pltpu.VMEM((8, 1024), F32),
            DMA((4,)), DMA((4,)),
            DMA((16,)), DMA((16,)), DMA((16,)), DMA((16,)), DMA((16,)), DMA((16,)),
            DMA((1,)), DMA((1,)), DMA((8,)), DMA((1,)), DMA((6,)),
        ],
        compiler_params=pltpu.CompilerParams(
            collective_id=1, has_side_effects=True, vmem_limit_bytes=60 * 1024 * 1024
        ),
        name="reduce",
    )(stiff, mass, diag, cm, rm)


def body(inv_interior, coupling, boundary_stiff, mass_interior, mass_boundary, block_map, modes):
    a2, b2, ma2, mb2, cm, rm = exchange(
        block_map, inv_interior, coupling, boundary_stiff, mass_interior, mass_boundary, modes.T
    )
    stiff_tile, mass_tile, diag = assemble(a2, b2, ma2, mb2)
    stiff, mass, diagonal = reduce_parts(
        stiff_tile, mass_tile, diag, cm.reshape(2, 1024, 1024), rm.reshape(1024, 1024)
    )
    return stiff_tile, mass_tile, stiff, mass, diagonal[0]


def solution(mesh):
    both = ("row", "col")
    return jax.shard_map(
        body,
        mesh=mesh,
        in_specs=(
            P(both, None, None),
            P(both, None, None),
            P(both, None, None),
            P(both, None),
            P(both, None),
            P(both, None),
            P("col", "row"),
        ),
        out_specs=(
            P("row", "col"),
            P("row", "col"),
            P(both, None),
            P(both, None),
            P(both),
        ),
        check_vma=False,
    )
```
